32 devices in a mesh: dp: 2 (over x), tp: 4 (over z), sp: 4 (over y, core).
Axes of the slice: x: 2, y: 2, z: 4, core: 2. Of those that a mesh axis runs over, the one named last changes fastest.
Arguments:
- x_tokens: bfloat16 [4096, 8192], P(('dp', 'sp'), 'tp'), parts along dimension 0
- doc_ids: int32 [4096], P(('dp', 'sp')), parts along dimension 0
- w_qkv: bfloat16 [8192, 24576], P('sp', 'tp')
- w_out: bfloat16 [8192, 8192], P('sp', 'tp')
Outputs:
- output: bfloat16 [4096, 8192], P(('dp', 'sp', 'tp')), parts along dimension 0
There are 2 independent parts. The reference program is written for one: setup_inputs(seed, part) draws one part's arguments, and reference() takes and returns one part's arrays. A program takes and returns all parts, laid end to end along the dimension named above; an argument that names none is the same for every part.
All inputs are finite; a program needn't handle non-finite values.
Results may differ from the reference program's by a relative error of at most 0.00292.
Values are sent between devices in bfloat16 or wider.
A program may use at most 1 GiB of HBM per device.

```python
import jax
import jax.numpy as jnp
from jax import lax

SEQ_LEN = 2048
HIDDEN = 8192
NUM_HEADS = 64
HEAD_DIM = 128
QUERY_BLOCK = 512
NUM_PIECES = 32
NUM_CUTS = 3

NUM_QBLOCKS = SEQ_LEN // QUERY_BLOCK
PIECE_LEN = SEQ_LEN // NUM_PIECES
SOFTMAX_SCALE = HEAD_DIM ** -0.5


def draw_segments(seg_key):
    cut_points = jax.random.randint(seg_key, (NUM_CUTS,), 1, SEQ_LEN)
    positions = jnp.arange(SEQ_LEN, dtype=jnp.int32)
    return jnp.sum((positions[:, None] >= cut_points[None, :]).astype(jnp.int32), axis=1).astype(jnp.int32)


def setup_inputs(seed: int = 0, part: int = 0) -> dict:
    base_key = jax.random.key(seed)
    part_key = jax.random.fold_in(base_key, part)
    noise_key, piece_key, seg_key = jax.random.split(part_key, 3)
    wqkv_key, wout_key = jax.random.split(jax.random.key(seed + 1), 2)
    x_noise = jax.random.normal(noise_key, (NUM_PIECES, PIECE_LEN, HIDDEN), jnp.float32)
    pieces = jax.random.normal(piece_key, (NUM_PIECES, 1, HIDDEN), jnp.float32)
    x_val = 0.6 * x_noise + 0.8 * pieces
    x_tokens = x_val.reshape(SEQ_LEN, HIDDEN).astype(jnp.bfloat16)
    w_qkv = (jax.random.normal(wqkv_key, (HIDDEN, 3 * HIDDEN), jnp.float32) * HIDDEN ** -0.5).astype(jnp.bfloat16)
    w_out = (jax.random.normal(wout_key, (HIDDEN, HIDDEN), jnp.float32) * (2.0 * HIDDEN ** -0.5)).astype(jnp.bfloat16)
    return {"x_tokens": x_tokens, "doc_ids": draw_segments(seg_key), "w_qkv": w_qkv, "w_out": w_out}


def reference(x_tokens, doc_ids, w_qkv, w_out):
    qkv_all = jnp.dot(x_tokens, w_qkv, preferred_element_type=jnp.float32).astype(jnp.bfloat16)
    per_head = qkv_all.reshape(SEQ_LEN, NUM_HEADS, 3, HEAD_DIM).transpose(1, 2, 0, 3).astype(jnp.float32)
    doc_blocks = doc_ids.reshape(NUM_QBLOCKS, QUERY_BLOCK)

    def head_attention(head_qkv):
        key_head = head_qkv[1]
        value_head = head_qkv[2]
        query_blocks = head_qkv[0].reshape(NUM_QBLOCKS, QUERY_BLOCK, HEAD_DIM)

        def block_attention(block):
            query_blk, doc_blk = block
            scores = jnp.dot(query_blk, key_head.T, preferred_element_type=jnp.float32) * SOFTMAX_SCALE
            same_doc = doc_blk[:, None] == doc_ids[None, :]
            scores = jnp.where(same_doc, scores, -jnp.inf)
            weights = jax.nn.softmax(scores, axis=-1).astype(jnp.bfloat16).astype(jnp.float32)
            return jnp.dot(weights, value_head, preferred_element_type=jnp.float32)

        context = lax.map(block_attention, (query_blocks, doc_blocks))
        return context.reshape(SEQ_LEN, HEAD_DIM).astype(jnp.bfloat16)

    context_all = lax.map(head_attention, per_head)
    context_all = context_all.transpose(1, 0, 2).reshape(SEQ_LEN, HIDDEN)
    return jnp.dot(context_all, w_out, preferred_element_type=jnp.float32).astype(jnp.bfloat16)
```

```python
import functools

import jax
import jax.numpy as jnp
from jax import lax
from jax.experimental import pallas as pl
from jax.experimental.pallas import tpu as pltpu
from jax.sharding import PartitionSpec as P

HEAD_DIM = 128
SOFTMAX_SCALE = HEAD_DIM ** -0.5
MESH = pl.DeviceIdType.MESH
VMEM_LIMIT = 67_000_000

PIECES = 4
FIRST = 2
WCHUNKS = 4


def sp_peers(sp):
    core = lax.rem(sp, 2)
    return sp + 1 - 2 * core, lax.rem(sp + 2, 4), 3 - sp


def send(src, dst, ssem, rsem, **device):
    copy = pltpu.make_async_remote_copy(
        src_ref=src, dst_ref=dst, send_sem=ssem, recv_sem=rsem, device_id=device, device_id_type=MESH
    )
    copy.start()


def wait_bytes(ref, sem):
    pltpu.make_async_copy(ref, ref, sem).wait()


def enter(peers):
    barrier = pltpu.get_barrier_semaphore()
    for peer in peers:
        pl.semaphore_signal(barrier, inc=1, device_id=peer, device_id_type=MESH)
    pl.semaphore_wait(barrier, len(peers))


def aligned(index, size):
    return pl.ds(pl.multiple_of(index * size, size), size)


def qkv_kernel(x_ref, seg_ref, w_ref, qkv_ref, segs_ref, xf, wf, stage,
               loc, ys, yr, zs, zr, xs, xr, ds, dr, gs, gr, outs):
    dp, z, sp = lax.axis_index("dp"), lax.axis_index("tp"), lax.axis_index("sp")
    cp, yp, ycp = sp_peers(sp)
    xp = 1 - dp
    rows, cols = x_ref.shape
    depth = w_ref.shape[0]
    group = w_ref.shape[1] // 4
    piece = rows // PIECES
    late = PIECES - FIRST
    items = PIECES + late
    half = depth // 2
    chunk = half // WCHUNKS

    enter([{"sp": cp}, {"sp": yp}, {"sp": ycp}, {"dp": xp}, {"tp": lax.rem(z + 1, 4)}, {"tp": lax.rem(z + 3, 4)}])

    def item_start(i, own, across):
        return own * PIECES + i if i < PIECES else across * PIECES + FIRST + i - PIECES

    def item_rows(i):
        return aligned(item_start(i, sp, yp), piece)

    def block(i, k):
        return xf.at[item_rows(i), aligned(k, cols)]

    def to_core(i, k):
        send(block(i, k), block(i, k), ds.at[i], dr.at[i], sp=cp)

    def z_send(i, d, s):
        if d == 0:
            @pl.when((z <= 2) & (z >= s - 1))
            def _():
                k = z - (s - 1)
                send(block(i, k), block(i, k), zs.at[i, d, s - 1], zr.at[i, d, s - 1], tp=z + 1)
        else:
            @pl.when((z >= 1) & (z + s - 1 <= 3))
            def _():
                k = z + (s - 1)
                send(block(i, k), block(i, k), zs.at[i, d, s - 1], zr.at[i, d, s - 1], tp=z - 1)

    def z_recv(i, s):
        @pl.when(z >= s)
        def _():
            wait_bytes(block(i, z - s), zr.at[i, 0, s - 1])
            if s < 3:
                z_send(i, 0, s + 1)
            to_core(i, z - s)

        @pl.when(z + s <= 3)
        def _():
            wait_bytes(block(i, z + s), zr.at[i, 1, s - 1])
            if s < 3:
                z_send(i, 1, s + 1)
            to_core(i, z + s)

    def w_rows(quarter, x_half, c):
        return aligned((quarter * 2 + x_half) * WCHUNKS + c, chunk)

    def w_recv(n):
        source = (yp, ycp)[n % 2]
        ref = wf.at[w_rows(source, dp, n // 2), :]
        wait_bytes(ref, yr.at[late + n])
        send(ref, ref, xs.at[n], xr.at[n % 2], dp=xp)

    x_own = pltpu.make_async_copy(x_ref, xf.at[aligned(sp, rows), aligned(z, cols)], loc.at[0])
    x_own.start()
    w_own = pltpu.make_async_copy(w_ref.at[:, aligned(sp, group)], wf.at[aligned(sp, depth), :], loc.at[1])
    w_own.start()
    seg_own = pltpu.make_async_copy(seg_ref, segs_ref.at[sp], loc.at[2])
    seg_own.start()
    for n, peer in enumerate((cp, yp, ycp)):
        send(seg_ref, segs_ref.at[sp], gs.at[n], gr.at[n], sp=peer)
    x_own.wait()
    for j in range(late):
        i = FIRST + j
        send(block(i, z), block(i, z), ys.at[j], yr.at[j], sp=yp)
    for n in range(2 * WCHUNKS):
        target = (yp, ycp)[n % 2]
        local = aligned(dp * WCHUNKS + n // 2, chunk)
        send(w_ref.at[local, aligned(target, group)], wf.at[w_rows(sp, dp, n // 2), :],
             ys.at[late + n], yr.at[late + n], sp=target)
    for i in range(PIECES):
        z_send(i, 0, 1)
        z_send(i, 1, 1)
    for i in range(PIECES):
        to_core(i, z)
    send(w_ref.at[:, aligned(cp, group)], wf.at[aligned(sp, depth), :], ds.at[items + FIRST], dr.at[items + FIRST], sp=cp)

    def y_recv(j):
        i = PIECES + j
        wait_bytes(block(i, z), yr.at[j])
        z_send(i, 0, 1)
        z_send(i, 1, 1)
        to_core(i, z)

    def q_send(i):
        ref = xf.at[item_rows(i), :]
        send(ref, ref, ys.at[late + 2 * WCHUNKS + i], yr.at[late + 2 * WCHUNKS + i], sp=yp)

    def q_rows(i, owner):
        return aligned(owner * PIECES + i, piece)

    def q_recv(i):
        ref = xf.at[q_rows(i, yp), :]
        wait_bytes(ref, yr.at[late + 2 * WCHUNKS + i])
        send(ref, ref, ds.at[items + i], dr.at[items + i], sp=cp)

    z_recv(0, 1)
    for j in range(late):
        y_recv(j)
    z_recv(1, 1)
    z_recv(2, 1)
    w_recv(0)
    z_recv(3, 1)
    w_recv(1)
    for i in range(PIECES, items):
        z_recv(i, 1)
    w_recv(2)
    z_recv(0, 2)
    z_recv(1, 2)
    w_recv(3)
    z_recv(2, 2)
    w_recv(4)
    z_recv(3, 2)
    w_recv(5)
    for i in range(PIECES, items):
        z_recv(i, 2)
    w_recv(6)
    for i in range(FIRST):
        z_recv(i, 3)
        q_send(i)
    w_recv(7)

    tile = 512 if group % 512 == 0 else group
    count = [0]

    def matmul(start, size):
        slot = count[0] % 2
        span = aligned(start, size)
        if count[0] >= 2:
            wait_bytes(stage.at[slot, pl.ds(0, sizes[count[0] - 2]), :], outs.at[slot])
        sizes.append(size)

        def step(n, carry):
            at = aligned(n, tile)
            stage[slot, 0:size, at] = jnp.dot(
                xf[span, :], wf[:, at], preferred_element_type=jnp.float32).astype(jnp.bfloat16)
            return carry

        lax.fori_loop(0, group // tile, step, 0)
        pltpu.make_async_copy(stage.at[slot, pl.ds(0, size), :], qkv_ref.at[span, :], outs.at[slot]).start()
        count[0] += 1

    sizes = []

    def core_rows(i):
        if i < items:
            return aligned(item_start(i, cp, ycp), piece)
        return q_rows(i - items, ycp)

    def from_core(i):
        wait_bytes(xf.at[core_rows(i), :], dr.at[i])

    w_own.wait()
    wait_bytes(wf.at[aligned(cp, depth), :], dr.at[items + FIRST])
    for n, source in enumerate((yp, ycp)):
        wait_bytes(wf.at[aligned(source * 2 + xp, half), :], xr.at[n])

    unit = FIRST * piece
    assert FIRST == late
    matmul(sp * 2, unit)
    for i in range(FIRST):
        from_core(i)
    for i in range(FIRST, PIECES):
        z_recv(i, 3)
    matmul(cp * 2, unit)
    for i in range(PIECES, items):
        z_recv(i, 3)
    matmul(sp * 2 + 1, unit)
    q_recv(0)
    for i in range(FIRST, PIECES):
        from_core(i)
    matmul(cp * 2 + 1, unit)
    for i in range(PIECES, items):
        from_core(i)
    matmul(yp * 2 + 1, unit)
    matmul(ycp * 2 + 1, unit)
    for i in range(1, FIRST):
        q_recv(i)
    matmul(yp * 2, unit)
    for i in range(FIRST):
        from_core(items + i)
    matmul(ycp * 2, unit)

    for slot in range(2):
        wait_bytes(stage.at[slot, pl.ds(0, unit), :], outs.at[slot])
    seg_own.wait()
    for n, peer in enumerate((cp, yp, ycp)):
        wait_bytes(seg_ref, gs.at[n])
        wait_bytes(segs_ref.at[peer], gr.at[n])
    for j in range(late):
        wait_bytes(block(FIRST + j, z), ys.at[j])
    for n in range(2 * WCHUNKS):
        ref = wf.at[pl.ds(0, chunk), :]
        wait_bytes(ref, ys.at[late + n])
        wait_bytes(ref, xs.at[n])
    for i in range(FIRST):
        wait_bytes(xf.at[item_rows(i), :], ys.at[late + 2 * WCHUNKS + i])
        wait_bytes(xf.at[q_rows(i, yp), :], ds.at[items + i])
    for i in range(items):
        wait_bytes(xf.at[item_rows(i), :], ds.at[i])
        for s in range(1, 4):
            @pl.when((z <= 2) & (z >= s - 1))
            def _():
                wait_bytes(block(i, z), zs.at[i, 0, s - 1])

            @pl.when((z >= 1) & (z + s - 1 <= 3))
            def _():
                wait_bytes(block(i, z), zs.at[i, 1, s - 1])
    wait_bytes(wf.at[aligned(sp, depth), :], ds.at[items + FIRST])


def gather_qkv(x, seg, w):
    rows, cols = x.shape
    depth, width = w.shape
    group = width // 4
    late = PIECES - FIRST
    items = PIECES + late
    crossings = late + 2 * WCHUNKS + FIRST
    dma = pltpu.SemaphoreType.DMA
    any_space = pl.BlockSpec(memory_space=pl.ANY)
    return pl.pallas_call(
        qkv_kernel,
        out_shape=(
            jax.ShapeDtypeStruct((4 * rows, group), jnp.bfloat16),
            jax.ShapeDtypeStruct((4,) + seg.shape, jnp.int32),
        ),
        in_specs=[any_space] * 3,
        out_specs=(any_space, any_space),
        scratch_shapes=[
            pltpu.VMEM((4 * rows, 4 * cols), jnp.bfloat16),
            pltpu.VMEM((4 * depth, group), jnp.bfloat16),
            pltpu.VMEM((2, FIRST * rows // PIECES, group), jnp.bfloat16),
            dma((3,)),
            dma((crossings,)),
            dma((crossings,)),
            dma((items, 2, 3)),
            dma((items, 2, 3)),
            dma((2 * WCHUNKS,)),
            dma((2,)),
            dma((items + FIRST + 1,)),
            dma((items + FIRST + 1,)),
            dma((3,)),
            dma((3,)),
            dma((2,)),
        ],
        compiler_params=pltpu.CompilerParams(collective_id=0, has_side_effects=True, vmem_limit_bytes=VMEM_LIMIT),
        name="gather_qkv",
    )(x, seg, w)


def attention_kernel(q_ref, k_ref, v_ref, segq_ref, segk_ref, o_ref):
    scores = lax.dot_general(q_ref[...], k_ref[...], (((1,), (1,)), ((), ())), preferred_element_type=jnp.float32)
    scores = jnp.where(segq_ref[...] == segk_ref[...], scores * SOFTMAX_SCALE, -jnp.inf)
    top = jnp.max(scores, axis=1, keepdims=True)
    weights = jnp.exp(scores - top)
    weights = (weights / jnp.sum(weights, axis=1, keepdims=True)).astype(jnp.bfloat16)
    o_ref[...] = jnp.dot(weights, v_ref[...], preferred_element_type=jnp.float32).astype(jnp.bfloat16)


def attention(qkv, segs):
    tokens, width = qkv.shape
    heads = width // (3 * HEAD_DIM)
    block = min(256, tokens)
    return pl.pallas_call(
        attention_kernel,
        out_shape=jax.ShapeDtypeStruct((tokens, heads * HEAD_DIM), jnp.bfloat16),
        grid=(heads, tokens // block),
        in_specs=[
            pl.BlockSpec((block, HEAD_DIM), lambda h, i: (i, 3 * h)),
            pl.BlockSpec((tokens, HEAD_DIM), lambda h, i: (0, 3 * h + 1)),
            pl.BlockSpec((tokens, HEAD_DIM), lambda h, i: (0, 3 * h + 2)),
            pl.BlockSpec((block, 1), lambda h, i: (i, 0)),
            pl.BlockSpec((1, tokens), lambda h, i: (0, 0)),
        ],
        out_specs=pl.BlockSpec((block, HEAD_DIM), lambda h, i: (i, h)),
        name="attention",
    )(qkv, qkv, qkv, segs.reshape(tokens, 1), segs.reshape(1, tokens))


def out_kernel(o_ref, w_ref, y_ref, of, wf, acc, stage,
               loc, os, orr, zs, zr, ys, yr, xs, xr, ds, dr, fs, fr, outl):
    dp, z, sp = lax.axis_index("dp"), lax.axis_index("tp"), lax.axis_index("sp")
    cp, yp, ycp = sp_peers(sp)
    xp = 1 - dp
    y = sp // 2
    tokens, width = o_ref.shape
    rows = tokens // 4
    depth, cols = w_ref.shape
    half = depth // 2
    chunk = half // WCHUNKS
    sources = (sp, cp, yp, ycp)

    enter([{"sp": cp}, {"sp": yp}, {"sp": ycp}, {"dp": xp}] + [{"tp": lax.rem(z + r, 4)} for r in (1, 2, 3)])

    def block(j, k):
        return of.at[:, aligned(k * 4 + sources[j], width)]

    def z_send(j, d, s):
        if d == 0:
            @pl.when((z <= 2) & (z >= s - 1))
            def _():
                k = z - (s - 1)
                send(block(j, k), block(j, k), zs.at[j, d, s - 1], zr.at[j, d, s - 1], tp=z + 1)
        else:
            @pl.when((z >= 1) & (z + s - 1 <= 3))
            def _():
                k = z + (s - 1)
                send(block(j, k), block(j, k), zs.at[j, d, s - 1], zr.at[j, d, s - 1], tp=z - 1)

    def z_recv(j, s):
        @pl.when(z >= s)
        def _():
            wait_bytes(block(j, z - s), zr.at[j, 0, s - 1])
            if s < 3:
                z_send(j, 0, s + 1)

        @pl.when(z + s <= 3)
        def _():
            wait_bytes(block(j, z + s), zr.at[j, 1, s - 1])
            if s < 3:
                z_send(j, 1, s + 1)

    def w_rows(quarter, x_half, c):
        return aligned((quarter * 2 + x_half) * WCHUNKS + c, chunk)

    def w_recv(n):
        ref = wf.at[w_rows(yp, dp, n), :]
        wait_bytes(ref, yr.at[n])
        send(ref, ref, xs.at[n], xr.at[n], dp=xp)
        send(ref, ref, ds.at[1], dr.at[1], sp=cp)

    def x_recv(n):
        ref = wf.at[w_rows(yp, xp, n), :]
        wait_bytes(ref, xr.at[n])
        send(ref, ref, ds.at[2], dr.at[2], sp=cp)

    o_own = pltpu.make_async_copy(o_ref.at[aligned(sp, rows), :], block(0, z), loc.at[0])
    o_own.start()
    for n, peer in enumerate((cp, yp, ycp)):
        send(o_ref.at[aligned(peer, rows), :], block(0, z), os.at[n], orr.at[n], sp=peer)
    for n in range(WCHUNKS):
        send(w_ref.at[aligned(dp * WCHUNKS + n, chunk), :], wf.at[w_rows(sp, dp, n), :], ys.at[n], yr.at[n], sp=yp)
    o_own.wait()
    z_send(0, 0, 1)
    z_send(0, 1, 1)
    w_own = pltpu.make_async_copy(w_ref, wf.at[aligned(sp, depth), :], loc.at[1])
    w_own.start()
    for n in range(3):
        wait_bytes(block(1 + n, z), orr.at[n])
        z_send(1 + n, 0, 1)
        z_send(1 + n, 1, 1)
        if n == 0:
            send(w_ref, wf.at[aligned(sp, depth), :], ds.at[0], dr.at[0], sp=cp)
            acc[...] = jnp.zeros_like(acc)
            z_recv(0, 1)
    z_recv(1, 1)
    z_recv(2, 1)
    w_recv(0)
    z_recv(3, 1)
    z_recv(0, 2)
    w_recv(1)
    z_recv(1, 2)
    x_recv(0)
    z_recv(2, 2)
    w_recv(2)
    z_recv(3, 2)
    x_recv(1)

    tile = min(512, cols)
    tiles = cols // tile

    def add_block(k):
        def step(n, carry):
            at = aligned(n, tile)
            acc[:, at] += jnp.dot(of[:, aligned(k, depth)], wf[aligned(k, depth), at],
                                  preferred_element_type=jnp.float32)
            return carry

        lax.fori_loop(0, tiles, step, 0)

    def near_blocks(when):
        for b in range(2):
            k = 2 * y + b

            @pl.when(when(k - z))
            def _():
                add_block(k)

    w_own.wait()
    wait_bytes(wf.at[aligned(cp, depth), :], dr.at[0])
    z_recv(0, 3)
    near_blocks(lambda gap: (gap <= 2) & (gap >= -2))
    w_recv(3)
    z_recv(1, 3)
    x_recv(2)
    z_recv(2, 3)
    x_recv(3)
    z_recv(3, 3)
    near_blocks(lambda gap: (gap > 2) | (gap < -2))
    for n in range(2):
        wait_bytes(wf.at[aligned(ycp * 2 + (dp, xp)[n], half), :], dr.at[1 + n])

    far = aligned(1 - y, 2 * depth)
    part = rows // 4
    for n in range(tiles):
        at = pl.ds(n * tile, tile)
        stage[:, at] = (acc[:, at] + jnp.dot(of[:, far], wf[far, at], preferred_element_type=jnp.float32)
                        ).astype(jnp.bfloat16)
        there = pl.ds(pl.multiple_of(z * cols + n * tile, tile), tile)
        for r in (2, 1, 3):
            to = lax.rem(z + r, 4)
            send(stage.at[aligned(to, part), at], y_ref.at[:, there], fs.at[r - 1], fr.at[r - 1], tp=to)
        pltpu.make_async_copy(stage.at[aligned(z, part), at], y_ref.at[:, there], outl.at[0]).start()

    for r in (1, 2, 3):
        source = lax.rem(z + 4 - r, 4)
        wait_bytes(y_ref.at[:, aligned(source, cols)], fr.at[r - 1])
        wait_bytes(stage.at[aligned(z, part), :], fs.at[r - 1])
    wait_bytes(y_ref.at[:, aligned(z, cols)], outl.at[0])
    for n, peer in enumerate((cp, yp, ycp)):
        wait_bytes(block(0, z), os.at[n])
    for n in range(WCHUNKS):
        ref = wf.at[pl.ds(0, chunk), :]
        wait_bytes(ref, ys.at[n])
        wait_bytes(ref, xs.at[n])
    wait_bytes(wf.at[aligned(sp, depth), :], ds.at[0])
    for n in range(2):
        wait_bytes(wf.at[aligned(yp * 2 + (dp, xp)[n], half), :], ds.at[1 + n])
    for j in range(4):
        for s in range(1, 4):
            @pl.when((z <= 2) & (z >= s - 1))
            def _():
                wait_bytes(block(j, z), zs.at[j, 0, s - 1])

            @pl.when((z >= 1) & (z + s - 1 <= 3))
            def _():
                wait_bytes(block(j, z), zs.at[j, 1, s - 1])


def project_out(o, w):
    tokens, width = o.shape
    rows = tokens // 4
    depth, cols = w.shape
    dma = pltpu.SemaphoreType.DMA
    any_space = pl.BlockSpec(memory_space=pl.ANY)
    return pl.pallas_call(
        out_kernel,
        out_shape=jax.ShapeDtypeStruct((rows // 4, 4 * cols), jnp.bfloat16),
        in_specs=[any_space] * 2,
        out_specs=any_space,
        scratch_shapes=[
            pltpu.VMEM((rows, 4 * depth), jnp.bfloat16),
            pltpu.VMEM((4 * depth, cols), jnp.bfloat16),
            pltpu.VMEM((rows, cols), jnp.float32),
            pltpu.VMEM((rows, cols), jnp.bfloat16),
            dma((2,)),
            dma((3,)),
            dma((3,)),
            dma((4, 2, 3)),
            dma((4, 2, 3)),
            dma((WCHUNKS,)),
            dma((WCHUNKS,)),
            dma((WCHUNKS,)),
            dma((WCHUNKS,)),
            dma((3,)),
            dma((3,)),
            dma((3,)),
            dma((3,)),
            dma((1,)),
        ],
        compiler_params=pltpu.CompilerParams(collective_id=1, has_side_effects=True, vmem_limit_bytes=VMEM_LIMIT),
        name="project_out",
    )(o, w)


def solution(mesh):
    shape = dict(mesh.shape)
    assert shape == {"dp": 2, "tp": 4, "sp": 4}

    def device_block(x_block, doc_block, wqkv_block, wout_block):
        qkv, segs = gather_qkv(x_block, doc_block.reshape(-1, HEAD_DIM), wqkv_block)
        return project_out(attention(qkv, segs), wout_block)

    return jax.shard_map(
        device_block,
        mesh=mesh,
        in_specs=(P(("dp", "sp"), "tp"), P(("dp", "sp")), P("sp", "tp"), P("sp", "tp")),
        out_specs=P(("dp", "sp", "tp"), None),
        check_vma=False,
    )
```

```python
import functools

import jax
import jax.numpy as jnp
from jax import lax
from jax.experimental import pallas as pl
from jax.experimental.pallas import tpu as pltpu
from jax.sharding import PartitionSpec as P

HEAD_DIM = 128
SOFTMAX_SCALE = HEAD_DIM ** -0.5
LOG2_E = 1.4426950408889634
MESH = pl.DeviceIdType.MESH
VMEM_LIMIT = 67_000_000

PIECES = 4
FIRST = 2
SHARES = (3, 3, 5, 5)
QKV_CHUNKS = 8
OUT_CHUNKS = 4


def sp_peers(sp):
    core = lax.rem(sp, 2)
    return sp + 1 - 2 * core, lax.rem(sp + 2, 4), 3 - sp


def send(src, dst, ssem, rsem, **device):
    copy = pltpu.make_async_remote_copy(
        src_ref=src, dst_ref=dst, send_sem=ssem, recv_sem=rsem, device_id=device, device_id_type=MESH
    )
    copy.start()


def wait_bytes(ref, sem):
    pltpu.make_async_copy(ref, ref, sem).wait()


def enter(peers):
    barrier = pltpu.get_barrier_semaphore()
    for peer in peers:
        pl.semaphore_signal(barrier, inc=1, device_id=peer, device_id_type=MESH)
    pl.semaphore_wait(barrier, len(peers))


def aligned(index, size):
    return pl.ds(pl.multiple_of(index * size, size), size)


def qkv_kernel(x_ref, seg_ref, w_ref, qkv_ref, segs_ref, xf, wf, stage,
               loc, ys, yr, zs, zr, xs, xr, ds, dr, gs, gr, outs):
    dp, z, sp = lax.axis_index("dp"), lax.axis_index("tp"), lax.axis_index("sp")
    cp, yp, ycp = sp_peers(sp)
    xp = 1 - dp
    rows, cols = x_ref.shape
    depth = w_ref.shape[0]
    group = w_ref.shape[1] // 4
    unit = rows // 16
    sizes = [share * unit for share in SHARES]
    offsets = [sum(sizes[:i]) for i in range(PIECES)]
    late = PIECES - FIRST
    items = PIECES + late
    half = depth // 2
    chunk = half // QKV_CHUNKS

    enter([{"sp": cp}, {"sp": yp}, {"sp": ycp}, {"dp": xp}, {"tp": lax.rem(z + 1, 4)}, {"tp": lax.rem(z + 3, 4)}])

    def span(owner, i, count=1):
        return pl.ds(pl.multiple_of(owner * rows + offsets[i], unit), sum(sizes[i:i + count]))

    def item_span(i, own, across):
        return span(own, i) if i < PIECES else span(across, FIRST + i - PIECES)

    def item_rows(i):
        return item_span(i, sp, yp)

    def block(i, k):
        return xf.at[item_rows(i), aligned(k, cols)]

    def to_core(i, k):
        send(block(i, k), block(i, k), ds.at[i], dr.at[i], sp=cp)

    def z_send(i, d, s):
        if d == 0:
            @pl.when((z <= 2) & (z >= s - 1))
            def _():
                k = z - (s - 1)
                send(block(i, k), block(i, k), zs.at[i, d, s - 1], zr.at[i, d, s - 1], tp=z + 1)
        else:
            @pl.when((z >= 1) & (z + s - 1 <= 3))
            def _():
                k = z + (s - 1)
                send(block(i, k), block(i, k), zs.at[i, d, s - 1], zr.at[i, d, s - 1], tp=z - 1)

    def z_recv(i, s):
        @pl.when(z >= s)
        def _():
            wait_bytes(block(i, z - s), zr.at[i, 0, s - 1])
            if s < 3:
                z_send(i, 0, s + 1)
            to_core(i, z - s)

        @pl.when(z + s <= 3)
        def _():
            wait_bytes(block(i, z + s), zr.at[i, 1, s - 1])
            if s < 3:
                z_send(i, 1, s + 1)
            to_core(i, z + s)

    def w_rows(quarter, x_half, c):
        return aligned((quarter * 2 + x_half) * QKV_CHUNKS + c, chunk)

    def w_recv(n):
        source = (yp, ycp)[n % 2]
        ref = wf.at[w_rows(source, dp, n // 2), :]
        wait_bytes(ref, yr.at[late + n])
        send(ref, ref, xs.at[n], xr.at[n % 2], dp=xp)

    x_own = pltpu.make_async_copy(x_ref, xf.at[aligned(sp, rows), aligned(z, cols)], loc.at[0])
    x_own.start()
    w_own = pltpu.make_async_copy(w_ref.at[:, aligned(sp, group)], wf.at[aligned(sp, depth), :], loc.at[1])
    w_own.start()
    seg_own = pltpu.make_async_copy(seg_ref, segs_ref.at[sp], loc.at[2])
    seg_own.start()
    for n, peer in enumerate((cp, yp, ycp)):
        send(seg_ref, segs_ref.at[sp], gs.at[n], gr.at[n], sp=peer)
    x_own.wait()
    for j in range(late):
        i = FIRST + j
        send(block(i, z), block(i, z), ys.at[j], yr.at[j], sp=yp)
    for n in range(2 * QKV_CHUNKS):
        target = (yp, ycp)[n % 2]
        local = aligned(dp * QKV_CHUNKS + n // 2, chunk)
        send(w_ref.at[local, aligned(target, group)], wf.at[w_rows(sp, dp, n // 2), :],
             ys.at[late + n], yr.at[late + n], sp=target)
    for i in range(PIECES):
        z_send(i, 0, 1)
        z_send(i, 1, 1)
    for i in range(PIECES):
        to_core(i, z)
    send(w_ref.at[:, aligned(cp, group)], wf.at[aligned(sp, depth), :], ds.at[items + FIRST], dr.at[items + FIRST], sp=cp)

    def y_recv(j):
        i = PIECES + j
        wait_bytes(block(i, z), yr.at[j])
        z_send(i, 0, 1)
        z_send(i, 1, 1)
        to_core(i, z)

    def q_send(i):
        ref = xf.at[item_rows(i), :]
        send(ref, ref, ys.at[late + 2 * QKV_CHUNKS + i], yr.at[late + 2 * QKV_CHUNKS + i], sp=yp)

    def q_recv(i):
        ref = xf.at[span(yp, i), :]
        wait_bytes(ref, yr.at[late + 2 * QKV_CHUNKS + i])
        send(ref, ref, ds.at[items + i], dr.at[items + i], sp=cp)

    z_recv(0, 1)
    for j in range(late):
        y_recv(j)
    z_recv(1, 1)
    w_recv(0)
    w_recv(1)
    z_recv(2, 1)
    w_recv(2)
    z_recv(3, 1)
    w_recv(3)
    w_recv(4)
    z_recv(4, 1)
    w_recv(5)
    z_recv(5, 1)
    w_recv(6)
    z_recv(0, 2)
    w_recv(7)
    z_recv(1, 2)
    w_recv(8)
    z_recv(2, 2)
    w_recv(9)
    z_recv(3, 2)
    w_recv(10)
    w_recv(11)
    z_recv(4, 2)
    w_recv(12)
    z_recv(5, 2)
    w_recv(13)
    z_recv(0, 3)
    q_send(0)
    w_recv(14)
    z_recv(1, 3)
    q_send(1)
    w_recv(15)

    tile = 512 if group % 512 == 0 else group
    done = []

    def matmul(where):
        slot = len(done) % 2
        if len(done) >= 2:
            wait_bytes(stage.at[slot, pl.ds(0, done[-2]), :], outs.at[slot])
        size = where.size
        done.append(size)

        def step(n, carry):
            at = aligned(n, tile)
            stage[slot, 0:size, at] = jnp.dot(
                xf[where, :], wf[:, at], preferred_element_type=jnp.float32).astype(jnp.bfloat16)
            return carry

        lax.fori_loop(0, group // tile, step, 0)
        pltpu.make_async_copy(stage.at[slot, pl.ds(0, size), :], qkv_ref.at[where, :], outs.at[slot]).start()

    def from_core(i):
        where = item_span(i, cp, ycp) if i < items else span(ycp, i - items)
        wait_bytes(xf.at[where, :], dr.at[i])

    w_own.wait()
    wait_bytes(wf.at[aligned(cp, depth), :], dr.at[items + FIRST])
    for n, source in enumerate((yp, ycp)):
        wait_bytes(wf.at[aligned(source * 2 + xp, half), :], xr.at[n])

    matmul(span(sp, 0, 2))
    z_recv(2, 3)
    for i in range(FIRST):
        from_core(i)
    matmul(span(cp, 0, 2))
    z_recv(3, 3)
    matmul(span(sp, 2, 2))
    q_recv(0)
    z_recv(4, 3)
    from_core(2)
    from_core(3)
    matmul(span(cp, 2, 2))
    z_recv(5, 3)
    from_core(4)
    matmul(span(yp, 2))
    matmul(span(ycp, 2))
    q_recv(1)
    from_core(5)
    matmul(span(yp, 3))
    matmul(span(ycp, 3))
    matmul(span(yp, 0, 2))
    from_core(items)
    from_core(items + 1)
    matmul(span(ycp, 0, 2))

    for back in (2, 1):
        slot = (len(done) - back) % 2
        wait_bytes(stage.at[slot, pl.ds(0, done[-back]), :], outs.at[slot])
    seg_own.wait()
    for n, peer in enumerate((cp, yp, ycp)):
        wait_bytes(seg_ref, gs.at[n])
        wait_bytes(segs_ref.at[peer], gr.at[n])
    for j in range(late):
        wait_bytes(block(FIRST + j, z), ys.at[j])
    for n in range(2 * QKV_CHUNKS):
        ref = wf.at[pl.ds(0, chunk), :]
        wait_bytes(ref, ys.at[late + n])
        wait_bytes(ref, xs.at[n])
    for i in range(FIRST):
        wait_bytes(xf.at[item_rows(i), :], ys.at[late + 2 * QKV_CHUNKS + i])
        wait_bytes(xf.at[span(yp, i), :], ds.at[items + i])
    for i in range(items):
        wait_bytes(xf.at[item_rows(i), :], ds.at[i])
        for s in range(1, 4):
            @pl.when((z <= 2) & (z >= s - 1))
            def _():
                wait_bytes(block(i, z), zs.at[i, 0, s - 1])

            @pl.when((z >= 1) & (z + s - 1 <= 3))
            def _():
                wait_bytes(block(i, z), zs.at[i, 1, s - 1])
    wait_bytes(wf.at[aligned(sp, depth), :], ds.at[items + FIRST])


def gather_qkv(x, seg, w):
    rows, cols = x.shape
    depth, width = w.shape
    group = width // 4
    late = PIECES - FIRST
    items = PIECES + late
    crossings = late + 2 * QKV_CHUNKS + FIRST
    dma = pltpu.SemaphoreType.DMA
    any_space = pl.BlockSpec(memory_space=pl.ANY)
    return pl.pallas_call(
        qkv_kernel,
        out_shape=(
            jax.ShapeDtypeStruct((4 * rows, group), jnp.bfloat16),
            jax.ShapeDtypeStruct((4,) + seg.shape, jnp.int32),
        ),
        in_specs=[any_space] * 3,
        out_specs=(any_space, any_space),
        scratch_shapes=[
            pltpu.VMEM((4 * rows, 4 * cols), jnp.bfloat16),
            pltpu.VMEM((4 * depth, group), jnp.bfloat16),
            pltpu.VMEM((2, rows * sum(SHARES[FIRST:]) // 16, group), jnp.bfloat16),
            dma((3,)),
            dma((crossings,)),
            dma((crossings,)),
            dma((items, 2, 3)),
            dma((items, 2, 3)),
            dma((2 * QKV_CHUNKS,)),
            dma((2,)),
            dma((items + FIRST + 1,)),
            dma((items + FIRST + 1,)),
            dma((3,)),
            dma((3,)),
            dma((2,)),
        ],
        compiler_params=pltpu.CompilerParams(collective_id=0, has_side_effects=True, vmem_limit_bytes=VMEM_LIMIT),
        name="gather_qkv",
    )(x, seg, w)


def attend(q, k, v, same):
    scores = lax.dot_general(q, k, (((1,), (1,)), ((), ())), preferred_element_type=jnp.float32)
    scores = jnp.where(same, scores, -jnp.inf)
    top = jnp.max(scores, axis=1, keepdims=True)
    weights = jnp.exp2((scores - top) * (SOFTMAX_SCALE * LOG2_E))
    inverse = 1.0 / jnp.sum(weights, axis=1, keepdims=True)
    weights = (weights * inverse).astype(jnp.bfloat16)
    return jnp.dot(weights, v, preferred_element_type=jnp.float32).astype(jnp.bfloat16)


def out_kernel(qkv_ref, segq_ref, segk_ref, w_ref, y_ref, qv, ov, of, wf, acc, stage,
               loc, os, orr, zs, zr, ys, yr, xs, xr, ds, dr, fs, fr, outl):
    dp, z, sp = lax.axis_index("dp"), lax.axis_index("tp"), lax.axis_index("sp")
    cp, yp, ycp = sp_peers(sp)
    xp = 1 - dp
    y = sp // 2
    tokens = qkv_ref.shape[0]
    width = qkv_ref.shape[1] // 3
    heads = width // HEAD_DIM
    rows = tokens // 4
    depth, cols = w_ref.shape
    half = depth // 2
    chunk = half // OUT_CHUNKS
    sources = (sp, cp, yp, ycp)

    qkv_in = pltpu.make_async_copy(qkv_ref, qv, loc.at[0])
    qkv_in.start()
    w_own = pltpu.make_async_copy(w_ref, wf.at[aligned(sp, depth), :], loc.at[1])
    w_own.start()
    enter([{"sp": cp}, {"sp": yp}, {"sp": ycp}, {"dp": xp}] + [{"tp": lax.rem(z + r, 4)} for r in (1, 2, 3)])

    def block(j, k):
        return of.at[:, aligned(k * 4 + sources[j], width)]

    def z_send(j, d, s):
        if d == 0:
            @pl.when((z <= 2) & (z >= s - 1))
            def _():
                k = z - (s - 1)
                send(block(j, k), block(j, k), zs.at[j, d, s - 1], zr.at[j, d, s - 1], tp=z + 1)
        else:
            @pl.when((z >= 1) & (z + s - 1 <= 3))
            def _():
                k = z + (s - 1)
                send(block(j, k), block(j, k), zs.at[j, d, s - 1], zr.at[j, d, s - 1], tp=z - 1)

    def z_recv(j, s):
        @pl.when(z >= s)
        def _():
            wait_bytes(block(j, z - s), zr.at[j, 0, s - 1])
            if s < 3:
                z_send(j, 0, s + 1)

        @pl.when(z + s <= 3)
        def _():
            wait_bytes(block(j, z + s), zr.at[j, 1, s - 1])
            if s < 3:
                z_send(j, 1, s + 1)

    def w_rows(quarter, x_half, c):
        return aligned((quarter * 2 + x_half) * OUT_CHUNKS + c, chunk)

    def w_recv(n):
        ref = wf.at[w_rows(yp, dp, n), :]
        wait_bytes(ref, yr.at[n])
        send(ref, ref, xs.at[n], xr.at[n], dp=xp)
        send(ref, ref, ds.at[1], dr.at[1], sp=cp)

    def x_recv(n):
        ref = wf.at[w_rows(yp, xp, n), :]
        wait_bytes(ref, xr.at[n])
        send(ref, ref, ds.at[2], dr.at[2], sp=cp)

    def w_send(n):
        send(w_ref.at[aligned(dp * OUT_CHUNKS + n, chunk), :], wf.at[w_rows(sp, dp, n), :], ys.at[n], yr.at[n], sp=yp)

    queries = min(256, rows)
    spans = rows // queries

    def attention(owner, store):
        def step(t, carry):
            h, b = t // spans, lax.rem(t, spans)
            at = aligned(owner * spans + b, queries)
            same = segq_ref[at, :] == segk_ref[...]
            store(h, aligned(b, queries), attend(
                qv[at, aligned(3 * h, HEAD_DIM)], qv[:, aligned(3 * h + 1, HEAD_DIM)],
                qv[:, aligned(3 * h + 2, HEAD_DIM)], same))
            return carry

        lax.fori_loop(0, heads * spans, step, 0)

    def store_own(h, at, value):
        of[at, aligned((z * 4 + sp) * heads + h, HEAD_DIM)] = value

    def attend_for(n):
        def store(h, at, value):
            ov[n, at, aligned(h, HEAD_DIM)] = value

        peer = sources[n + 1]
        attention(peer, store)
        send(ov.at[n], block(0, z), os.at[n], orr.at[n], sp=peer)

    def o_recv(n):
        wait_bytes(block(1 + n, z), orr.at[n])
        z_send(1 + n, 0, 1)
        z_send(1 + n, 1, 1)

    w_send(0)
    send(w_ref, wf.at[aligned(sp, depth), :], ds.at[0], dr.at[0], sp=cp)
    qkv_in.wait()
    attention(sp, store_own)
    z_send(0, 0, 1)
    z_send(0, 1, 1)
    attend_for(1)
    z_recv(0, 1)
    attend_for(2)
    for n in range(1, OUT_CHUNKS):
        w_send(n)
    o_recv(1)
    attend_for(0)
    o_recv(2)
    o_recv(0)
    w_recv(0)
    z_recv(0, 2)
    acc[...] = jnp.zeros_like(acc)
    z_recv(2, 1)
    z_recv(0, 3)
    z_recv(3, 1)
    w_recv(1)
    z_recv(1, 1)
    x_recv(0)
    z_recv(2, 2)
    z_recv(3, 2)
    w_recv(2)
    x_recv(1)
    z_recv(1, 2)

    tile = min(512, cols)
    tiles = cols // tile

    def add_block(k):
        def step(n, carry):
            at = aligned(n, tile)
            acc[:, at] += jnp.dot(of[:, aligned(k, depth)], wf[aligned(k, depth), at],
                                  preferred_element_type=jnp.float32)
            return carry

        lax.fori_loop(0, tiles, step, 0)

    def near_blocks(when):
        for b in range(2):
            k = 2 * y + b

            @pl.when(when(k - z))
            def _():
                add_block(k)

    w_own.wait()
    wait_bytes(wf.at[aligned(cp, depth), :], dr.at[0])
    near_blocks(lambda gap: (gap <= 2) & (gap >= -2))
    z_recv(2, 3)
    w_recv(3)
    x_recv(2)
    z_recv(3, 3)
    x_recv(3)
    z_recv(1, 3)
    near_blocks(lambda gap: (gap > 2) | (gap < -2))
    for n in range(2):
        wait_bytes(wf.at[aligned(ycp * 2 + (dp, xp)[n], half), :], dr.at[1 + n])

    far = aligned(1 - y, 2 * depth)
    part = rows // 4
    for n in range(tiles):
        at = pl.ds(n * tile, tile)
        stage[:, at] = (acc[:, at] + jnp.dot(of[:, far], wf[far, at], preferred_element_type=jnp.float32)
                        ).astype(jnp.bfloat16)
        there = pl.ds(pl.multiple_of(z * cols + n * tile, tile), tile)
        for r in (2, 1, 3):
            to = lax.rem(z + r, 4)
            send(stage.at[aligned(to, part), at], y_ref.at[:, there], fs.at[r - 1], fr.at[r - 1], tp=to)
        pltpu.make_async_copy(stage.at[aligned(z, part), at], y_ref.at[:, there], outl.at[0]).start()

    for r in (1, 2, 3):
        source = lax.rem(z + 4 - r, 4)
        wait_bytes(y_ref.at[:, aligned(source, cols)], fr.at[r - 1])
        wait_bytes(stage.at[aligned(z, part), :], fs.at[r - 1])
    wait_bytes(y_ref.at[:, aligned(z, cols)], outl.at[0])
    for n, peer in enumerate((cp, yp, ycp)):
        wait_bytes(ov.at[n], os.at[n])
    for n in range(OUT_CHUNKS):
        ref = wf.at[pl.ds(0, chunk), :]
        wait_bytes(ref, ys.at[n])
        wait_bytes(ref, xs.at[n])
    wait_bytes(wf.at[aligned(sp, depth), :], ds.at[0])
    for n in range(2):
        wait_bytes(wf.at[aligned(yp * 2 + (dp, xp)[n], half), :], ds.at[1 + n])
    for j in range(4):
        for s in range(1, 4):
            @pl.when((z <= 2) & (z >= s - 1))
            def _():
                wait_bytes(block(j, z), zs.at[j, 0, s - 1])

            @pl.when((z >= 1) & (z + s - 1 <= 3))
            def _():
                wait_bytes(block(j, z), zs.at[j, 1, s - 1])


def attend_project(qkv, segs, w):
    tokens, width = qkv.shape[0], qkv.shape[1] // 3
    rows = tokens // 4
    depth, cols = w.shape
    dma = pltpu.SemaphoreType.DMA
    any_space = pl.BlockSpec(memory_space=pl.ANY)
    return pl.pallas_call(
        out_kernel,
        out_shape=jax.ShapeDtypeStruct((rows // 4, 4 * cols), jnp.bfloat16),
        in_specs=[any_space] + [pl.BlockSpec(memory_space=pltpu.VMEM)] * 2 + [any_space],
        out_specs=any_space,
        scratch_shapes=[
            pltpu.VMEM(qkv.shape, jnp.bfloat16),
            pltpu.VMEM((3, rows, width), jnp.bfloat16),
            pltpu.VMEM((rows, 4 * depth), jnp.bfloat16),
            pltpu.VMEM((4 * depth, cols), jnp.bfloat16),
            pltpu.VMEM((rows, cols), jnp.float32),
            pltpu.VMEM((rows, cols), jnp.bfloat16),
            dma((2,)),
            dma((3,)),
            dma((3,)),
            dma((4, 2, 3)),
            dma((4, 2, 3)),
            dma((OUT_CHUNKS,)),
            dma((OUT_CHUNKS,)),
            dma((OUT_CHUNKS,)),
            dma((OUT_CHUNKS,)),
            dma((3,)),
            dma((3,)),
            dma((3,)),
            dma((3,)),
            dma((1,)),
        ],
        compiler_params=pltpu.CompilerParams(collective_id=1, has_side_effects=True, vmem_limit_bytes=VMEM_LIMIT),
        name="attend_project",
    )(qkv, segs.reshape(tokens, 1), segs.reshape(1, tokens), w)


def solution(mesh):
    shape = dict(mesh.shape)
    assert shape == {"dp": 2, "tp": 4, "sp": 4}

    def device_block(x_block, doc_block, wqkv_block, wout_block):
        qkv, segs = gather_qkv(x_block, doc_block.reshape(-1, HEAD_DIM), wqkv_block)
        return attend_project(qkv, segs, wout_block)

    return jax.shard_map(
        device_block,
        mesh=mesh,
        in_specs=(P(("dp", "sp"), "tp"), P(("dp", "sp")), P("sp", "tp"), P("sp", "tp")),
        out_specs=P(("dp", "sp", "tp"), None),
        check_vma=False,
    )
```

```python
import jax
import jax.numpy as jnp
from jax import lax
from jax.experimental import pallas as pl
from jax.experimental.pallas import tpu as pltpu
from jax.sharding import PartitionSpec as P

HEAD_DIM = 128
HEAD_COLS = 3 * HEAD_DIM
SOFTMAX_SCALE = HEAD_DIM ** -0.5
LOG2_E = 1.4426950408889634
MESH = pl.DeviceIdType.MESH
VMEM_LIMIT = 67_000_000

PIECES = 4
FIRST = 2
SHARES = (5, 4, 4, 3)
HEADS = 4
GROUPS = ((0, 2), (2, 1), (3, 1))
CHUNKS = (4, 2, 2)
W_BASE = (0, 8, 12)
TILES = 4
QKV_STEPS = 8


def send(src, dst, ssem, rsem, **device):
    copy = pltpu.make_async_remote_copy(
        src_ref=src, dst_ref=dst, send_sem=ssem, recv_sem=rsem, device_id=device, device_id_type=MESH
    )
    copy.start()


def local(src, dst, sem):
    copy = pltpu.make_async_copy(src, dst, sem)
    copy.start()
    return copy


def wait_bytes(ref, sem):
    pltpu.make_async_copy(ref, ref, sem).wait()


def enter(peers):
    barrier = pltpu.get_barrier_semaphore()
    for peer in peers:
        pl.semaphore_signal(barrier, inc=1, device_id=peer, device_id_type=MESH)
    pl.semaphore_wait(barrier, len(peers))


def aligned(index, size):
    return pl.ds(pl.multiple_of(index * size, size), size)


def columns(start, size):
    return pl.ds(pl.multiple_of(start, HEAD_DIM), size)


def attend(q, k, v, same):
    scores = lax.dot_general(q, k, (((1,), (1,)), ((), ())), preferred_element_type=jnp.float32)
    scores = jnp.where(same, scores, -jnp.inf)
    top = jnp.max(scores, axis=1, keepdims=True)
    weights = jnp.exp2((scores - top) * (SOFTMAX_SCALE * LOG2_E))
    inverse = 1.0 / jnp.sum(weights, axis=1, keepdims=True)
    weights = (weights * inverse).astype(jnp.bfloat16)
    return jnp.dot(weights, v, preferred_element_type=jnp.float32).astype(jnp.bfloat16)


def block_kernel(x_ref, seg_ref, w_ref, wo_ref, y_ref, xall, woall,
                 xs, wf, qv, of, ov, stage, segs, segcol, segrow,
                 loc, seg_s, seg_r, xy_s, xy_r, xz_s, xz_r, xd_s, xd_r,
                 wy_s, wy_r, wx_s, wx_r, wd_s, wd_r,
                 op_s, op_r, oz_s, oz_r,
                 vy_s, vy_r, vx_s, vx_r, vd_s, vd_r, vl, f_s, f_r):
    dp, z, sp = lax.axis_index("dp"), lax.axis_index("tp"), lax.axis_index("sp")
    core, y = lax.rem(sp, 2), sp // 2
    cp, yp, ycp = sp + 1 - 2 * core, lax.rem(sp + 2, 4), 3 - sp
    xp = 1 - dp
    sources = (sp, cp, yp, ycp)
    rows, cols = x_ref.shape
    tokens = 4 * rows
    depth = w_ref.shape[0]
    half = depth // 2
    width = HEADS * HEAD_DIM
    unit = rows // 16
    sizes = [share * unit for share in SHARES]
    offsets = [sum(sizes[:i]) for i in range(PIECES)]
    late = PIECES - FIRST
    items = PIECES + late

    def span(owner, i, count=1):
        return pl.ds(pl.multiple_of(owner * rows + offsets[i], unit), sum(sizes[i:i + count]))

    def item_span(i, own, across):
        return span(own, i) if i < PIECES else span(across, FIRST + i - PIECES)

    def x_block(i, k):
        return xall.at[item_span(i, sp, yp), aligned(k, cols)]

    def x_source(i, k, own):
        return x_ref.at[pl.ds(offsets[i], sizes[i]), :] if own and i < PIECES else x_block(i, k)

    def x_core(i, k, own=False):
        send(x_source(i, k, own), x_block(i, k), xd_s.at[i], xd_r.at[i], sp=cp)

    def line_send(copy, s_sem, r_sem, d, s):
        if d == 0:
            @pl.when((z <= 2) & (z >= s - 1))
            def _():
                k = z - (s - 1)
                send(copy[0](k), copy[1](k), s_sem.at[d, s - 1], r_sem.at[d, s - 1], tp=z + 1)
        else:
            @pl.when((z >= 1) & (z + s - 1 <= 3))
            def _():
                k = z + (s - 1)
                send(copy[0](k), copy[1](k), s_sem.at[d, s - 1], r_sem.at[d, s - 1], tp=z - 1)

    def x_line(i, d, s):
        line_send((lambda k: x_source(i, k, s == 1), lambda k: x_block(i, k)), xz_s.at[i], xz_r.at[i], d, s)

    def x_first(i):
        x_line(i, 0, 1)
        x_line(i, 1, 1)

    def x_recv(i, s):
        @pl.when(z >= s)
        def _():
            wait_bytes(x_block(i, z - s), xz_r.at[i, 0, s - 1])
            if s < 3:
                x_line(i, 0, s + 1)
            x_core(i, z - s)

        @pl.when(z + s <= 3)
        def _():
            wait_bytes(x_block(i, z + s), xz_r.at[i, 1, s - 1])
            if s < 3:
                x_line(i, 1, s + 1)
            x_core(i, z + s)

    def p_recv(j):
        wait_bytes(x_block(PIECES + j, z), xy_r.at[j])
        x_core(PIECES + j, z)

    def q_send(i):
        ref = xall.at[span(sp, i), :]
        send(ref, ref, xy_s.at[late + i], xy_r.at[late + i], sp=yp)

    def q_recv(i):
        ref = xall.at[span(yp, i), :]
        wait_bytes(ref, xy_r.at[late + i])
        send(ref, ref, xd_s.at[items + i], xd_r.at[items + i], sp=cp)

    def from_core(i):
        where = item_span(i, cp, ycp) if i < items else span(ycp, i - items)
        wait_bytes(xall.at[where, :], xd_r.at[i])

    def group_cols(g, owner=0):
        first, count = GROUPS[g]
        return columns((owner * HEADS + first) * HEAD_COLS, count * HEAD_COLS)

    def w_rows(quarter, x_half, g, c):
        return aligned((quarter * 2 + x_half) * CHUNKS[g] + c, half // CHUNKS[g])

    def w_send(g):
        for c in range(2 * CHUNKS[g]):
            target = (yp, ycp)[c % 2]
            send(w_ref.at[aligned(dp * CHUNKS[g] + c // 2, half // CHUNKS[g]), group_cols(g, target)],
                 wf.at[w_rows(sp, dp, g, c // 2), group_cols(g)],
                 wy_s.at[W_BASE[g] + c], wy_r.at[W_BASE[g] + c], sp=target)

    def w_recv(g, c):
        ref = wf.at[w_rows((yp, ycp)[c % 2], dp, g, c // 2), group_cols(g)]
        wait_bytes(ref, wy_r.at[W_BASE[g] + c])
        send(ref, ref, wx_s.at[W_BASE[g] + c], wx_r.at[2 * g + c % 2], dp=xp)

    def w_ready(g):
        for n, source in enumerate((yp, ycp)):
            wait_bytes(wf.at[aligned(source * 2 + xp, half), group_cols(g)], wx_r.at[2 * g + n])

    split = (columns(0, 2 * HEAD_COLS), columns(2 * HEAD_COLS, 2 * HEAD_COLS))

    def w_core(n):
        send(w_ref.at[:, columns((cp * HEADS + 2 * n) * HEAD_COLS, 2 * HEAD_COLS)],
             wf.at[aligned(sp, depth), split[n]], wd_s.at[n], wd_r.at[n], sp=cp)

    def w_from_core(n):
        wait_bytes(wf.at[aligned(cp, depth), split[n]], wd_r.at[n])

    def load(where, slot):
        local(xall.at[where, :], xs.at[slot, pl.ds(0, where.size), :], loc.at[4 + slot])

    def go(where, slot):
        size = where.size
        wait_bytes(xs.at[slot, pl.ds(0, size), :], loc.at[4 + slot])

        def step(n, carry):
            at = aligned(n, 2 * HEAD_DIM)
            qv[where, at] = jnp.dot(xs[slot, 0:size, :], wf[0:4 * depth, at],
                                    preferred_element_type=jnp.float32).astype(jnp.bfloat16)
            return carry

        lax.fori_loop(0, GROUPS[0][1] * HEAD_COLS // (2 * HEAD_DIM), step, 0)

    def qkv(where, slot):
        load(where, slot)
        go(where, slot)

    def at_step(n, events):
        for k, acts in events.items():
            @pl.when(n == k)
            def _():
                for act, *args in acts:
                    act(*args)

    part = tokens // QKV_STEPS

    def qkv_group(g, events):
        first, count = GROUPS[g]
        at = pl.ds(first * HEAD_COLS, count * HEAD_COLS)
        load(aligned(0, part), 0)

        def step(n, carry):
            slot = lax.rem(n, 2)

            @pl.when(n + 1 < QKV_STEPS)
            def _():
                local(xall.at[aligned(n + 1, part), :], xs.at[1 - slot, pl.ds(0, part), :], loc.at[5 - slot])

            wait_bytes(xs.at[slot, pl.ds(0, part), :], loc.at[4 + slot])
            qv[aligned(n, part), at] = jnp.dot(xs[slot, 0:part, :], wf[0:4 * depth, at],
                                               preferred_element_type=jnp.float32).astype(jnp.bfloat16)
            at_step(n, events)
            return carry

        lax.fori_loop(0, QKV_STEPS, step, 0)

    def o_block(g, j, k):
        first, count = GROUPS[g]
        return of.at[:, columns(((k * 4 + sources[j]) * HEADS + first) * HEAD_DIM, count * HEAD_DIM)]

    def o_line(g, j, d, s):
        item = 4 * g + j
        line_send((lambda k: o_block(g, j, k),) * 2, oz_s.at[item], oz_r.at[item], d, s)

    def o_first(g, j):
        o_line(g, j, 0, 1)
        o_line(g, j, 1, 1)

    def o_recv(g, j):
        wait_bytes(o_block(g, j, z), op_r.at[3 * g + j - 1])
        o_first(g, j)

    def o_next(g, j, s):
        @pl.when(z >= s)
        def _():
            wait_bytes(o_block(g, j, z - s), oz_r.at[4 * g + j, 0, s - 1])
            if s < 3:
                o_line(g, j, 0, s + 1)

        @pl.when(z + s <= 3)
        def _():
            wait_bytes(o_block(g, j, z + s), oz_r.at[4 * g + j, 1, s - 1])
            if s < 3:
                o_line(g, j, 1, s + 1)

    queries = min(256, rows)
    spans = rows // queries
    order = (0, 2, 3, 1)

    def attention(g, events):
        first, count = GROUPS[g]
        here = pl.ds(first * HEAD_DIM, count * HEAD_DIM)

        def quarter(n, carry):
            owner = 2 * lax.rem(y + lax.rem((n + 1) // 2, 2), 2) + lax.rem(core + n // 2, 2)

            def step(t, carry):
                h, b = first + t // spans, lax.rem(t, spans)
                at = aligned(owner * spans + b, queries)
                ov[n, aligned(b, queries), aligned(h, HEAD_DIM)] = attend(
                    qv[at, aligned(3 * h, HEAD_DIM)], qv[:, aligned(3 * h + 1, HEAD_DIM)],
                    qv[:, aligned(3 * h + 2, HEAD_DIM)], segcol[at, 0:1] == segrow[...])
                return carry

            lax.fori_loop(0, count * spans, step, 0)

            @pl.when(n == 0)
            def _():
                of[:, columns(((z * 4 + sp) * HEADS + first) * HEAD_DIM, count * HEAD_DIM)] = ov[0, :, here]
                o_first(g, 0)

            for k in range(1, 4):
                @pl.when(n == k)
                def _():
                    j = order[k]
                    send(ov.at[k, :, here], o_block(g, 0, z), op_s.at[3 * g + j - 1], op_r.at[3 * g + j - 1],
                         sp=sources[j])

            at_step(n, events)
            return carry

        lax.fori_loop(0, 4, quarter, 0)

    o_depth, out_cols = wo_ref.shape
    o_half = o_depth // 2
    tile = out_cols // TILES

    def v_block(quarter, x_half, c):
        return (aligned((quarter * 2 + x_half) * 2 + c % 2, o_half // 2), pl.ds(c // 2 * tile, tile))

    def v_send(c):
        at = v_block(sp, dp, c)
        send(wo_ref.at[aligned(dp * 2 + c % 2, o_half // 2), pl.ds(c // 2 * tile, tile)], woall.at[at],
             vy_s.at[c], vy_r.at[c], sp=yp)

    def v_recv(c):
        ref = woall.at[v_block(yp, dp, c)]
        wait_bytes(ref, vy_r.at[c])
        send(ref, ref, vx_s.at[c], vx_r.at[c], dp=xp)
        send(ref, ref, vd_s.at[c // 2], vd_r.at[c // 2], sp=cp)

    def v_from_x(c):
        ref = woall.at[v_block(yp, xp, c)]
        wait_bytes(ref, vx_r.at[c])
        send(ref, ref, vd_s.at[c // 2], vd_r.at[c // 2], sp=cp)

    def v_place(t):
        return pl.ds(t % 3 * tile, tile)

    def v_load(t):
        at = pl.ds(t * tile, tile)
        wait_bytes(woall.at[aligned(ycp, o_depth), at], vd_r.at[t])
        local(wo_ref.at[:, at], wf.at[aligned(sp, o_depth), v_place(t)], vl.at[t])
        for source in (cp, yp, ycp):
            local(woall.at[aligned(source, o_depth), at], wf.at[aligned(source, o_depth), v_place(t)], vl.at[t])

    piece = rows // 4
    narrow = min(tile, 2 * HEAD_DIM)

    def project(t):
        wait_bytes(wf.at[pl.ds(0, 4 * o_depth), v_place(t)], vl.at[t])

        def step(n, carry):
            stage[:, columns(t * tile + n * narrow, narrow)] = jnp.dot(
                of[...], wf[0:4 * o_depth, columns(t % 3 * tile + n * narrow, narrow)],
                preferred_element_type=jnp.float32).astype(jnp.bfloat16)
            return carry

        lax.fori_loop(0, tile // narrow, step, 0)
        at = pl.ds(t * tile, tile)
        there = columns(z * out_cols + t * tile, tile)
        for r in (2, 1, 3):
            to = lax.rem(z + r, 4)
            send(stage.at[aligned(to, piece), at], y_ref.at[:, there], f_s.at[r - 1], f_r.at[r - 1], tp=to)
        local(stage.at[aligned(z, piece), at], y_ref.at[:, there], loc.at[6])

    x_in = local(x_ref, stage.at[:, pl.ds(0, cols)], loc.at[0])
    w_own = local(w_ref.at[:, columns(sp * HEADS * HEAD_COLS, HEADS * HEAD_COLS)], wf.at[aligned(sp, depth), :],
                  loc.at[2])
    seg_own = local(seg_ref, segs.at[sp], loc.at[3])
    enter([{"sp": cp}, {"sp": yp}, {"sp": ycp}, {"dp": xp}] + [{"tp": lax.rem(z + r, 4)} for r in (1, 2, 3)])
    for j in range(late):
        i = FIRST + j
        send(x_source(i, z, True), x_block(i, z), xy_s.at[j], xy_r.at[j], sp=yp)
    for i in range(FIRST):
        x_first(i)
    w_send(0)
    for n, peer in enumerate((cp, yp, ycp)):
        send(seg_ref, segs.at[sp], seg_s.at[n], seg_r.at[n], sp=peer)
    for i in range(PIECES):
        x_core(i, z, True)
    w_core(0)
    x_in.wait()
    x_put = local(stage.at[:, pl.ds(0, cols)], xall.at[aligned(sp, rows), aligned(z, cols)], loc.at[1])

    seg_own.wait()
    for n, peer in enumerate((cp, yp, ycp)):
        wait_bytes(segs.at[peer], seg_r.at[n])
    seg_rows = rows // HEAD_DIM
    for q in range(4):
        for r in range(seg_rows):
            line = segs[q, r:r + 1, :]
            at = (q * seg_rows + r) * HEAD_DIM
            segrow[:, at:at + HEAD_DIM] = line
            segcol[at:at + HEAD_DIM, :] = jnp.broadcast_to(line, (HEAD_DIM, HEAD_DIM)).T
    x_put.wait()

    x_recv(0, 1)
    p_recv(0)
    p_recv(1)
    x_recv(1, 1)
    w_recv(0, 0)
    w_recv(0, 1)
    x_recv(0, 2)
    w_recv(0, 2)
    x_recv(1, 2)
    for i in range(FIRST, items):
        x_first(i)
    w_recv(0, 3)
    w_recv(0, 4)
    x_recv(0, 3)
    q_send(0)
    w_recv(0, 5)
    x_recv(1, 3)
    q_send(1)
    w_send(1)
    w_recv(0, 6)
    w_recv(0, 7)
    w_core(1)
    w_own.wait()
    w_from_core(0)
    w_ready(0)
    qkv(span(sp, 0, 2), 0)
    x_recv(2, 1)
    x_recv(3, 1)
    from_core(0)
    from_core(1)
    qkv(span(cp, 0, 2), 1)
    x_recv(4, 1)
    x_recv(5, 1)
    x_recv(2, 2)
    x_recv(3, 2)
    q_recv(0)
    x_recv(4, 2)
    x_recv(5, 2)
    qkv(span(yp, 0), 0)
    from_core(items)
    qkv(span(ycp, 0), 1)
    x_recv(2, 3)
    x_recv(3, 3)
    from_core(2)
    from_core(3)
    qkv(span(sp, 2, 2), 0)
    qkv(span(cp, 2, 2), 1)
    x_recv(4, 3)
    q_recv(1)
    load(span(yp, 1), 0)
    x_recv(5, 3)
    load(span(yp, 2, 2), 1)
    go(span(yp, 1), 0)
    from_core(items + 1)
    load(span(ycp, 1), 0)
    go(span(yp, 2, 2), 1)
    from_core(4)
    from_core(5)
    load(span(ycp, 2, 2), 1)
    go(span(ycp, 1), 0)
    go(span(ycp, 2, 2), 1)

    attention(0, {
        0: [(w_recv, 1, 0), (w_recv, 1, 1)],
        1: [(o_next, 0, 0, 1), (w_recv, 1, 2)],
        2: [(w_send, 2), (o_next, 0, 0, 2), (w_recv, 1, 3)],
    })
    o_recv(0, 2)
    o_recv(0, 1)
    o_next(0, 0, 3)
    o_recv(0, 3)
    w_from_core(1)
    w_ready(1)
    qkv_group(1, {
        0: [(o_next, 0, 2, 1)],
        1: [(o_next, 0, 1, 1)],
        3: [(o_next, 0, 3, 1)],
        4: [(w_recv, 2, 0)],
        5: [(o_next, 0, 2, 2)],
        6: [(w_recv, 2, 1)],
        7: [(o_next, 0, 1, 2)],
    })
    attention(1, {
        0: [(w_recv, 2, 2)],
        2: [(v_send, 0), (v_send, 1), (v_send, 2)],
        3: [(o_next, 0, 3, 2), (w_recv, 2, 3)],
    })
    send(wo_ref, woall.at[aligned(sp, o_depth), :], vd_s.at[TILES], vd_r.at[TILES], sp=cp)
    o_next(0, 2, 3)
    o_recv(1, 1)
    o_recv(1, 2)
    o_next(0, 1, 3)
    o_recv(1, 3)
    w_ready(2)
    qkv_group(2, {
        0: [(o_next, 0, 3, 3)],
        1: [(o_next, 1, 0, 1)],
        2: [(o_next, 1, 1, 1)],
        3: [(o_next, 1, 2, 1)],
        4: [(o_next, 1, 3, 1), (v_recv, 0)],
        5: [(o_next, 1, 0, 2)],
        6: [(o_next, 1, 1, 2)],
        7: [(o_next, 1, 2, 2)],
    })
    attention(2, {
        0: [(v_recv, 1)],
        1: [(o_next, 1, 3, 2)],
        2: [(v_send, 3), (v_send, 4), (v_send, 5), (v_send, 6), (v_send, 7)],
        3: [(o_next, 1, 0, 3), (v_recv, 2)],
    })
    o_recv(2, 1)
    o_next(1, 1, 3)
    o_next(1, 2, 3)
    o_recv(2, 2)
    o_recv(2, 3)
    o_next(1, 3, 3)

    for c in range(W_BASE[2] + 2 * CHUNKS[2]):
        g = max(g for g in range(3) if W_BASE[g] <= c)
        wait_bytes(wf.at[pl.ds(0, half // CHUNKS[g]), group_cols(g)], wx_s.at[c])
    wait_bytes(woall.at[aligned(cp, o_depth), :], vd_r.at[TILES])
    for j in range(4):
        o_next(2, j, 1)
    v_from_x(0)
    v_from_x(1)
    v_load(0)
    v_recv(3)
    for j in range(4):
        o_next(2, j, 2)
    v_recv(4)
    v_from_x(2)
    v_from_x(3)
    v_load(1)
    for j in range(4):
        o_next(2, j, 3)
    v_recv(5)
    project(0)
    v_from_x(4)
    v_from_x(5)
    v_load(2)
    v_recv(6)
    project(1)
    v_recv(7)
    project(2)
    v_from_x(6)
    v_from_x(7)
    v_load(3)
    project(3)

    for r in (1, 2, 3):
        wait_bytes(y_ref.at[:, aligned(lax.rem(z + 4 - r, 4), out_cols)], f_r.at[r - 1])
        wait_bytes(stage.at[aligned(z, piece), :], f_s.at[r - 1])
    wait_bytes(y_ref.at[:, aligned(z, out_cols)], loc.at[6])
    for n in range(3):
        wait_bytes(seg_ref, seg_s.at[n])
    for j in range(late):
        wait_bytes(x_block(FIRST + j, z), xy_s.at[j])
    for i in range(FIRST):
        wait_bytes(xall.at[span(sp, i), :], xy_s.at[late + i])
        wait_bytes(xall.at[span(yp, i), :], xd_s.at[items + i])
    for c in range(W_BASE[2] + 2 * CHUNKS[2]):
        g = max(g for g in range(3) if W_BASE[g] <= c)
        wait_bytes(wf.at[pl.ds(0, half // CHUNKS[g]), group_cols(g)], wy_s.at[c])
    for n in range(2):
        wait_bytes(wf.at[aligned(sp, depth), split[n]], wd_s.at[n])
    for c in range(2 * TILES):
        ref = woall.at[v_block(yp, dp, c)]
        wait_bytes(ref, vy_s.at[c])
        wait_bytes(ref, vx_s.at[c])
    for t in range(TILES):
        wait_bytes(woall.at[aligned(yp, o_depth), pl.ds(t * tile, tile)], vd_s.at[t])
    wait_bytes(wo_ref, vd_s.at[TILES])
    for g in range(3):
        first, count = GROUPS[g]
        for k in range(1, 4):
            wait_bytes(ov.at[k, :, pl.ds(first * HEAD_DIM, count * HEAD_DIM)], op_s.at[3 * g + order[k] - 1])

    def sent(ref, sems):
        for s in range(1, 4):
            @pl.when((z <= 2) & (z >= s - 1))
            def _():
                wait_bytes(ref, sems.at[0, s - 1])

            @pl.when((z >= 1) & (z + s - 1 <= 3))
            def _():
                wait_bytes(ref, sems.at[1, s - 1])

    for i in range(items):
        wait_bytes(xall.at[item_span(i, sp, yp), :], xd_s.at[i])
        sent(x_block(i, z), xz_s.at[i])
    for g in range(3):
        for j in range(4):
            sent(o_block(g, j, z), oz_s.at[4 * g + j])


def attention_block(x, seg, w, wo):
    rows, cols = x.shape
    depth, group = w.shape[0], w.shape[1] // 4
    o_depth, out_cols = wo.shape
    tokens = 4 * rows
    unit = rows // 16
    items = 2 * PIECES - FIRST
    width = HEADS * HEAD_DIM
    chunks = W_BASE[2] + 2 * CHUNKS[2]
    any_space = pl.BlockSpec(memory_space=pl.ANY)
    longest = max(SHARES[0] + SHARES[1], sum(SHARES[FIRST:])) * unit
    longest = max(longest, tokens // QKV_STEPS)

    def dma(*shape):
        return pltpu.SemaphoreType.DMA(shape)

    y, _, _ = pl.pallas_call(
        block_kernel,
        out_shape=(
            jax.ShapeDtypeStruct((rows // 4, 4 * out_cols), jnp.bfloat16),
            jax.ShapeDtypeStruct((tokens, 4 * cols), jnp.bfloat16),
            jax.ShapeDtypeStruct((4 * o_depth, out_cols), jnp.bfloat16),
        ),
        in_specs=[any_space] * 4,
        out_specs=(any_space,) * 3,
        scratch_shapes=[
            pltpu.VMEM((2, longest, 4 * cols), jnp.bfloat16),
            pltpu.VMEM((4 * max(depth, o_depth), group), jnp.bfloat16),
            pltpu.VMEM((tokens, group), jnp.bfloat16),
            pltpu.VMEM((rows, 4 * o_depth), jnp.bfloat16),
            pltpu.VMEM((4, rows, width), jnp.bfloat16),
            pltpu.VMEM((rows, max(cols, out_cols)), jnp.bfloat16),
            pltpu.VMEM((4,) + seg.shape, jnp.int32),
            pltpu.VMEM((tokens, HEAD_DIM), jnp.int32),
            pltpu.VMEM((1, tokens), jnp.int32),
            dma(7),
            dma(3), dma(3),
            dma(PIECES), dma(PIECES), dma(items, 2, 3), dma(items, 2, 3), dma(items + FIRST), dma(items + FIRST),
            dma(chunks), dma(chunks), dma(chunks), dma(6), dma(2), dma(2),
            dma(9), dma(9), dma(12, 2, 3), dma(12, 2, 3),
            dma(2 * TILES), dma(2 * TILES), dma(2 * TILES), dma(2 * TILES), dma(TILES + 1), dma(TILES + 1), dma(TILES),
            dma(3), dma(3),
        ],
        compiler_params=pltpu.CompilerParams(collective_id=0, has_side_effects=True, vmem_limit_bytes=VMEM_LIMIT),
        name="attention_block",
    )(x, seg, w, wo)
    return y


def solution(mesh):
    shape = dict(mesh.shape)
    assert shape == {"dp": 2, "tp": 4, "sp": 4}

    def device_block(x_block, doc_block, wqkv_block, wout_block):
        return attention_block(x_block, doc_block.reshape(-1, HEAD_DIM), wqkv_block, wout_block)

    return jax.shard_map(
        device_block,
        mesh=mesh,
        in_specs=(P(("dp", "sp"), "tp"), P(("dp", "sp")), P("sp", "tp"), P("sp", "tp")),
        out_specs=P(("dp", "sp", "tp"), None),
        check_vma=False,
    )
```

```python
import jax
import jax.numpy as jnp
from jax import lax
from jax.experimental import pallas as pl
from jax.experimental.pallas import tpu as pltpu
from jax.sharding import PartitionSpec as P

HEAD_DIM = 128
HEAD_COLS = 3 * HEAD_DIM
SOFTMAX_SCALE = HEAD_DIM ** -0.5
LOG2_E = 1.4426950408889634
MESH = pl.DeviceIdType.MESH
VMEM_LIMIT = 67_000_000

PIECES = 4
FIRST = 2
SHARES = (5, 4, 4, 3)
HEADS = 4
GROUPS = ((0, 2), (2, 1), (3, 1))
CHUNKS = (4, 2, 2)
W_BASE = (0, 8, 12)
TILES = 4
QKV_STEPS = 8


def scoped(f):
    def wrapped(*args):
        tag = "_".join(str(a) for a in args if isinstance(a, int))
        with jax.named_scope(f.__name__ + "_" + tag):
            return f(*args)
    return wrapped


def send(src, dst, ssem, rsem, **device):
    copy = pltpu.make_async_remote_copy(
        src_ref=src, dst_ref=dst, send_sem=ssem, recv_sem=rsem, device_id=device, device_id_type=MESH
    )
    copy.start()


def local(src, dst, sem):
    copy = pltpu.make_async_copy(src, dst, sem)
    copy.start()
    return copy


def wait_bytes(ref, sem):
    pltpu.make_async_copy(ref, ref, sem).wait()


@scoped
def enter(peers):
    barrier = pltpu.get_barrier_semaphore()
    for peer in peers:
        pl.semaphore_signal(barrier, inc=1, device_id=peer, device_id_type=MESH)
    pl.semaphore_wait(barrier, len(peers))


def aligned(index, size):
    return pl.ds(pl.multiple_of(index * size, size), size)


def columns(start, size):
    return pl.ds(pl.multiple_of(start, HEAD_DIM), size)


def attend(q, k, v, same):
    scores = lax.dot_general(q, k, (((1,), (1,)), ((), ())), preferred_element_type=jnp.float32)
    scores = jnp.where(same, scores, -jnp.inf)
    top = jnp.max(scores, axis=1, keepdims=True)
    weights = jnp.exp2((scores - top) * (SOFTMAX_SCALE * LOG2_E))
    inverse = 1.0 / jnp.sum(weights, axis=1, keepdims=True)
    weights = (weights * inverse).astype(jnp.bfloat16)
    return jnp.dot(weights, v, preferred_element_type=jnp.float32).astype(jnp.bfloat16)


def block_kernel(x_ref, seg_ref, w_ref, wo_ref, y_ref, xall, woall,
                 xs, wf, qv, of, ov, stage, segs, segcol, segrow,
                 loc, seg_s, seg_r, xy_s, xy_r, xz_s, xz_r, xd_s, xd_r,
                 wy_s, wy_r, wx_s, wx_r, wd_s, wd_r,
                 op_s, op_r, oz_s, oz_r,
                 vy_s, vy_r, vx_s, vx_r, vd_s, vd_r, vl, f_s, f_r):
    dp, z, sp = lax.axis_index("dp"), lax.axis_index("tp"), lax.axis_index("sp")
    core, y = lax.rem(sp, 2), sp // 2
    cp, yp, ycp = sp + 1 - 2 * core, lax.rem(sp + 2, 4), 3 - sp
    xp = 1 - dp
    sources = (sp, cp, yp, ycp)
    steps = (1, 2, 3)
    rows, cols = x_ref.shape
    tokens = 4 * rows
    depth = w_ref.shape[0]
    half = depth // 2
    width = HEADS * HEAD_DIM
    unit = rows // 16
    sizes = [share * unit for share in SHARES]
    offsets = [sum(sizes[:i]) for i in range(PIECES)]
    late = PIECES - FIRST
    items = PIECES + late

    def span(owner, i, count=1):
        return pl.ds(pl.multiple_of(owner * rows + offsets[i], unit), sum(sizes[i:i + count]))

    def item_span(i, own, across):
        return span(own, i) if i < PIECES else span(across, FIRST + i - PIECES)

    def x_block(i, k):
        return xall.at[item_span(i, sp, yp), aligned(k, cols)]

    def x_source(i, k, own):
        return x_ref.at[pl.ds(offsets[i], sizes[i]), :] if own and i < PIECES else x_block(i, k)

    def x_core(i, k, own=False):
        send(x_source(i, k, own), x_block(i, k), xd_s.at[i], xd_r.at[i], sp=cp)

    def line_send(copy, s_sem, r_sem, d, s):
        if d == 0:
            @pl.when((z <= 2) & (z >= s - 1))
            def _():
                k = z - (s - 1)
                send(copy[0](k), copy[1](k), s_sem.at[d, s - 1], r_sem.at[d, s - 1], tp=z + 1)
        else:
            @pl.when((z >= 1) & (z + s - 1 <= 3))
            def _():
                k = z + (s - 1)
                send(copy[0](k), copy[1](k), s_sem.at[d, s - 1], r_sem.at[d, s - 1], tp=z - 1)

    def x_line(i, d, s):
        line_send((lambda k: x_source(i, k, s == 1), lambda k: x_block(i, k)), xz_s.at[i], xz_r.at[i], d, s)

    def x_first(i):
        x_line(i, 0, 1)
        x_line(i, 1, 1)

    @scoped
    def x_recv(i, s):
        @pl.when(z >= s)
        def _():
            wait_bytes(x_block(i, z - s), xz_r.at[i, 0, s - 1])
            if s < 3:
                x_line(i, 0, s + 1)
            x_core(i, z - s)

        @pl.when(z + s <= 3)
        def _():
            wait_bytes(x_block(i, z + s), xz_r.at[i, 1, s - 1])
            if s < 3:
                x_line(i, 1, s + 1)
            x_core(i, z + s)

    @scoped
    def p_recv(j):
        wait_bytes(x_block(PIECES + j, z), xy_r.at[j])
        x_core(PIECES + j, z)

    def q_send(i):
        ref = xall.at[span(sp, i), :]
        send(ref, ref, xy_s.at[late + i], xy_r.at[late + i], sp=yp)

    @scoped
    def q_recv(i):
        ref = xall.at[span(yp, i), :]
        wait_bytes(ref, xy_r.at[late + i])
        send(ref, ref, xd_s.at[items + i], xd_r.at[items + i], sp=cp)

    @scoped
    def from_core(i):
        where = item_span(i, cp, ycp) if i < items else span(ycp, i - items)
        wait_bytes(xall.at[where, :], xd_r.at[i])

    def group_cols(g, owner=0):
        first, count = GROUPS[g]
        return columns((owner * HEADS + first) * HEAD_COLS, count * HEAD_COLS)

    def w_rows(quarter, x_half, g, c):
        return aligned((quarter * 2 + x_half) * CHUNKS[g] + c, half // CHUNKS[g])

    def w_send(g):
        for c in range(2 * CHUNKS[g]):
            target = (yp, ycp)[c % 2]
            send(w_ref.at[aligned(dp * CHUNKS[g] + c // 2, half // CHUNKS[g]), group_cols(g, target)],
                 wf.at[w_rows(sp, dp, g, c // 2), group_cols(g)],
                 wy_s.at[W_BASE[g] + c], wy_r.at[W_BASE[g] + c], sp=target)

    @scoped
    def w_recv(g, c):
        ref = wf.at[w_rows((yp, ycp)[c % 2], dp, g, c // 2), group_cols(g)]
        wait_bytes(ref, wy_r.at[W_BASE[g] + c])
        send(ref, ref, wx_s.at[W_BASE[g] + c], wx_r.at[2 * g + c % 2], dp=xp)

    @scoped
    def w_ready(g):
        for n, source in enumerate((yp, ycp)):
            wait_bytes(wf.at[aligned(source * 2 + xp, half), group_cols(g)], wx_r.at[2 * g + n])

    split = (columns(0, 2 * HEAD_COLS), columns(2 * HEAD_COLS, 2 * HEAD_COLS))

    def w_core(n):
        send(w_ref.at[:, columns((cp * HEADS + 2 * n) * HEAD_COLS, 2 * HEAD_COLS)],
             wf.at[aligned(sp, depth), split[n]], wd_s.at[n], wd_r.at[n], sp=cp)

    @scoped
    def w_from_core(n):
        wait_bytes(wf.at[aligned(cp, depth), split[n]], wd_r.at[n])

    @scoped
    def load(where, slot):
        local(xall.at[where, :], xs.at[slot, pl.ds(0, where.size), :], loc.at[4 + slot])

    @scoped
    def go(where, slot):
        size = where.size
        wait_bytes(xs.at[slot, pl.ds(0, size), :], loc.at[4 + slot])

        def step(n, carry):
            at = aligned(n, 2 * HEAD_DIM)
            qv[where, at] = jnp.dot(xs[slot, 0:size, :], wf[0:4 * depth, at],
                                    preferred_element_type=jnp.float32).astype(jnp.bfloat16)
            return carry

        lax.fori_loop(0, GROUPS[0][1] * HEAD_COLS // (2 * HEAD_DIM), step, 0)

    def qkv(where, slot):
        load(where, slot)
        go(where, slot)

    def at_step(n, events):
        for k, acts in events.items():
            @pl.when(n == k)
            def _():
                for act, *args in acts:
                    act(*args)

    part = tokens // QKV_STEPS

    @scoped
    def qkv_group(g, events):
        first, count = GROUPS[g]
        at = pl.ds(first * HEAD_COLS, count * HEAD_COLS)
        load(aligned(0, part), 0)

        def step(n, carry):
            slot = lax.rem(n, 2)

            @pl.when(n + 1 < QKV_STEPS)
            def _():
                local(xall.at[aligned(n + 1, part), :], xs.at[1 - slot, pl.ds(0, part), :], loc.at[5 - slot])

            wait_bytes(xs.at[slot, pl.ds(0, part), :], loc.at[4 + slot])
            qv[aligned(n, part), at] = jnp.dot(xs[slot, 0:part, :], wf[0:4 * depth, at],
                                               preferred_element_type=jnp.float32).astype(jnp.bfloat16)
            at_step(n, events)
            return carry

        lax.fori_loop(0, QKV_STEPS, step, 0)

    def o_block(g, j, k):
        first, count = GROUPS[g]
        return of.at[:, columns(((k * 4 + sources[j]) * HEADS + first) * HEAD_DIM, count * HEAD_DIM)]

    def o_line(g, j, d, s):
        item = 4 * g + j
        line_send((lambda k: o_block(g, j, k),) * 2, oz_s.at[item], oz_r.at[item], d, s)

    def o_first(g, j):
        o_line(g, j, 0, 1)
        o_line(g, j, 1, 1)

    @scoped
    def o_recv(g, j):
        wait_bytes(o_block(g, j, z), op_r.at[3 * g + j - 1])
        o_first(g, j)

    @scoped
    def o_next(g, j, s):
        @pl.when(z >= s)
        def _():
            wait_bytes(o_block(g, j, z - s), oz_r.at[4 * g + j, 0, s - 1])
            if s < 3:
                o_line(g, j, 0, s + 1)

        @pl.when(z + s <= 3)
        def _():
            wait_bytes(o_block(g, j, z + s), oz_r.at[4 * g + j, 1, s - 1])
            if s < 3:
                o_line(g, j, 1, s + 1)

    queries = min(256, rows)
    spans = rows // queries
    order = (0, 2, 3, 1)

    @scoped
    def attention(g, events):
        first, count = GROUPS[g]
        here = pl.ds(first * HEAD_DIM, count * HEAD_DIM)

        def quarter(n, carry):
            owner = 2 * lax.rem(y + lax.rem((n + 1) // 2, 2), 2) + lax.rem(core + n // 2, 2)

            def step(t, carry):
                h, b = first + t // spans, lax.rem(t, spans)
                at = aligned(owner * spans + b, queries)
                ov[n, aligned(b, queries), aligned(h, HEAD_DIM)] = attend(
                    qv[at, aligned(3 * h, HEAD_DIM)], qv[:, aligned(3 * h + 1, HEAD_DIM)],
                    qv[:, aligned(3 * h + 2, HEAD_DIM)], segcol[at, 0:1] == segrow[...])
                return carry

            with jax.named_scope("att"):
                lax.fori_loop(0, count * spans, step, 0)

            @pl.when(n == 0)
            def _():
                of[:, columns(((z * 4 + sp) * HEADS + first) * HEAD_DIM, count * HEAD_DIM)] = ov[0, :, here]
                o_first(g, 0)

            for k in range(1, 4):
                @pl.when(n == k)
                def _():
                    j = order[k]
                    send(ov.at[k, :, here], o_block(g, 0, z), op_s.at[3 * g + j - 1], op_r.at[3 * g + j - 1],
                         sp=sources[j])

            at_step(n, events)
            return carry

        lax.fori_loop(0, 4, quarter, 0)

    o_depth, out_cols = wo_ref.shape
    o_half = o_depth // 2
    tile = out_cols // TILES

    def v_block(quarter, x_half, c):
        return (aligned((quarter * 2 + x_half) * 2 + c % 2, o_half // 2), pl.ds(c // 2 * tile, tile))

    def v_send(c):
        at = v_block(sp, dp, c)
        send(wo_ref.at[aligned(dp * 2 + c % 2, o_half // 2), pl.ds(c // 2 * tile, tile)], woall.at[at],
             vy_s.at[c], vy_r.at[c], sp=yp)

    @scoped
    def v_recv(c):
        ref = woall.at[v_block(yp, dp, c)]
        wait_bytes(ref, vy_r.at[c])
        send(ref, ref, vx_s.at[c], vx_r.at[c], dp=xp)
        send(ref, ref, vd_s.at[c // 2], vd_r.at[c // 2], sp=cp)

    @scoped
    def v_from_x(c):
        ref = woall.at[v_block(yp, xp, c)]
        wait_bytes(ref, vx_r.at[c])
        send(ref, ref, vd_s.at[c // 2], vd_r.at[c // 2], sp=cp)

    def v_place(t):
        return pl.ds(t % 3 * tile, tile)

    @scoped
    def v_load(t):
        at = pl.ds(t * tile, tile)
        wait_bytes(woall.at[aligned(ycp, o_depth), at], vd_r.at[t])
        local(wo_ref.at[:, at], wf.at[aligned(sp, o_depth), v_place(t)], vl.at[t])
        for source in (cp, yp, ycp):
            local(woall.at[aligned(source, o_depth), at], wf.at[aligned(source, o_depth), v_place(t)], vl.at[t])

    piece = rows // 4
    narrow = min(tile, 2 * HEAD_DIM)

    @scoped
    def project(t):
        wait_bytes(wf.at[pl.ds(0, 4 * o_depth), v_place(t)], vl.at[t])

        def step(n, carry):
            stage[:, columns(t * tile + n * narrow, narrow)] = jnp.dot(
                of[...], wf[0:4 * o_depth, columns(t % 3 * tile + n * narrow, narrow)],
                preferred_element_type=jnp.float32).astype(jnp.bfloat16)
            return carry

        lax.fori_loop(0, tile // narrow, step, 0)
        at = pl.ds(t * tile, tile)
        there = columns(z * out_cols + t * tile, tile)
        for r in (2, 1, 3):
            to = lax.rem(z + r, 4)
            send(stage.at[aligned(to, piece), at], y_ref.at[:, there], f_s.at[r - 1], f_r.at[r - 1], tp=to)
        local(stage.at[aligned(z, piece), at], y_ref.at[:, there], loc.at[6])

    x_in = local(x_ref, stage.at[:, pl.ds(0, cols)], loc.at[0])
    w_own = local(w_ref.at[:, columns(sp * HEADS * HEAD_COLS, HEADS * HEAD_COLS)], wf.at[aligned(sp, depth), :],
                  loc.at[2])
    seg_own = local(seg_ref, segs.at[sp], loc.at[3])
    enter([{"sp": cp}, {"sp": yp}, {"sp": ycp}, {"dp": xp}] + [{"tp": lax.rem(z + r, 4)} for r in (1, 2, 3)])
    for n, peer in enumerate((cp, yp, ycp)):
        send(seg_ref, segs.at[sp], seg_s.at[n], seg_r.at[n], sp=peer)
    for j in range(late):
        i = FIRST + j
        send(x_source(i, z, True), x_block(i, z), xy_s.at[j], xy_r.at[j], sp=yp)
    for i in range(FIRST):
        x_first(i)
    w_send(0)
    for i in range(PIECES):
        x_core(i, z, True)
    w_core(0)
    x_in.wait()
    x_put = local(stage.at[:, pl.ds(0, cols)], xall.at[aligned(sp, rows), aligned(z, cols)], loc.at[1])

    x_put.wait()

    chunk = iter(range(2 * CHUNKS[0]))
    for s in steps:
        for i in range(FIRST):
            x_recv(i, s)
            if s == 1:
                p_recv(i)
            else:
                w_recv(0, next(chunk))
            if s == 2:
                w_recv(0, next(chunk))
            if s == 3:
                q_send(i)
        if s == 2:
            for i in range(FIRST, items):
                x_first(i)
    w_send(1)
    for c in chunk:
        w_recv(0, c)
    w_core(1)
    w_own.wait()
    w_from_core(0)
    w_ready(0)
    seg_own.wait()
    for n, peer in enumerate((cp, yp, ycp)):
        wait_bytes(segs.at[peer], seg_r.at[n])
    seg_rows = rows // HEAD_DIM
    for q in range(4):
        for r in range(seg_rows):
            line = segs[q, r:r + 1, :]
            at = (q * seg_rows + r) * HEAD_DIM
            segrow[:, at:at + HEAD_DIM] = line
            segcol[at:at + HEAD_DIM, :] = jnp.broadcast_to(line, (HEAD_DIM, HEAD_DIM)).T
    early = range(FIRST)
    after = range(FIRST, PIECES)
    across = range(PIECES, items)
    qkv(span(sp, 0, FIRST), 0)
    for i in after:
        x_recv(i, 1)
    for i in early:
        from_core(i)
    qkv(span(cp, 0, FIRST), 1)
    for i in across:
        x_recv(i, 1)
    for i in after:
        x_recv(i, 2)
    q_recv(0)
    for i in across:
        x_recv(i, 2)
    qkv(span(yp, 0), 0)
    from_core(items)
    qkv(span(ycp, 0), 1)
    for i in after:
        x_recv(i, 3)
    for i in after:
        from_core(i)
    qkv(span(sp, FIRST, late), 0)
    qkv(span(cp, FIRST, late), 1)
    x_recv(across[0], 3)
    q_recv(1)
    load(span(yp, 1), 0)
    load(span(yp, 2), 1)
    go(span(yp, 1), 0)
    from_core(items + 1)
    load(span(ycp, 1), 0)
    go(span(yp, 2), 1)
    from_core(across[0])
    load(span(ycp, 2), 1)
    x_recv(across[1], 3)
    go(span(ycp, 1), 0)
    load(span(yp, 3), 0)
    go(span(ycp, 2), 1)
    from_core(across[1])
    load(span(ycp, 3), 1)
    go(span(yp, 3), 0)
    go(span(ycp, 3), 1)

    def spread(start, every, acts):
        return {start + every * i: [act] for i, act in enumerate(acts)}

    def weights(g):
        return [(w_recv, g, c) for c in range(2 * CHUNKS[g])]

    def pieces(g, upto):
        return [(o_next, g, j, s) for s in range(1, upto + 1) for j in order]

    def run(acts):
        for act, *args in acts:
            act(*args)

    own = [(o_next, 0, 0, s) for s in steps]
    rest = [(o_next, 0, j, s) for s in steps for j in order[1:]]
    chunks = weights(1)
    attention(0, {0: chunks[:2], 1: own[:1] + chunks[2:3], 2: [(w_send, 2)] + own[1:2] + chunks[3:]})
    for j in order[1:3]:
        o_recv(0, j)
    run(own[2:])
    o_recv(0, order[3])
    w_from_core(1)
    w_ready(1)
    chunks = weights(2)
    qkv_group(1, spread(0, 2, rest[:4]) | spread(3, 2, chunks[:2]))
    rest = rest[4:]
    wo_chunks = [(v_send, c) for c in range(2 * TILES)]
    attention(1, {0: chunks[2:3], 2: wo_chunks[:3] + chunks[3:], 3: rest[:2]})
    send(wo_ref, woall.at[aligned(sp, o_depth), :], vd_s.at[TILES], vd_r.at[TILES], sp=cp)
    run(rest[2:3])
    for j in (1, 2, 3):
        o_recv(1, j)
    run(rest[3:-1])
    w_ready(2)
    follow = rest[-1:] + pieces(1, 3)
    blocks = [(v_recv, c) for c in range(2 * TILES)]
    plan = spread(0, 1, follow[:QKV_STEPS])
    plan[4] += blocks[:1]
    qkv_group(2, plan)
    follow = follow[QKV_STEPS:]
    attention(2, {0: blocks[1:2], 1: follow[:1], 2: wo_chunks[3:], 3: follow[1:2] + blocks[2:3]})
    run(follow[2:-1])
    for j in order[:0:-1]:
        o_recv(2, j)
    run(follow[-1:])

    crossed = [(W_BASE[g] + c, g) for g in range(len(GROUPS)) for c in range(2 * CHUNKS[g])]
    for c, g in crossed:
        wait_bytes(wf.at[pl.ds(0, half // CHUNKS[g]), group_cols(g)], wx_s.at[c])
    wait_bytes(woall.at[aligned(cp, o_depth), :], vd_r.at[TILES])

    def ready(t):
        v_from_x(2 * t)
        v_from_x(2 * t + 1)
        v_load(t)

    follow = pieces(2, 3)
    run(follow[:4])
    ready(0)
    run(blocks[3:4] + follow[4:8] + blocks[4:5])
    ready(1)
    run(follow[8:10] + blocks[5:6] + follow[10:])
    project(0)
    run(blocks[6:7])
    project(1)
    ready(2)
    run(blocks[7:])
    project(2)
    ready(3)
    project(3)

    for r in (1, 2, 3):
        wait_bytes(y_ref.at[:, aligned(lax.rem(z + 4 - r, 4), out_cols)], f_r.at[r - 1])
        wait_bytes(stage.at[aligned(z, piece), :], f_s.at[r - 1])
    wait_bytes(y_ref.at[:, aligned(z, out_cols)], loc.at[6])
    for n in range(3):
        wait_bytes(seg_ref, seg_s.at[n])
    for j in range(late):
        wait_bytes(x_block(FIRST + j, z), xy_s.at[j])
    for i in range(FIRST):
        wait_bytes(xall.at[span(sp, i), :], xy_s.at[late + i])
        wait_bytes(xall.at[span(yp, i), :], xd_s.at[items + i])
    for c, g in crossed:
        wait_bytes(wf.at[pl.ds(0, half // CHUNKS[g]), group_cols(g)], wy_s.at[c])
    for n in range(2):
        wait_bytes(wf.at[aligned(sp, depth), split[n]], wd_s.at[n])
    for c in range(2 * TILES):
        ref = woall.at[v_block(yp, dp, c)]
        wait_bytes(ref, vy_s.at[c])
        wait_bytes(ref, vx_s.at[c])
    for t in range(TILES):
        wait_bytes(woall.at[aligned(yp, o_depth), pl.ds(t * tile, tile)], vd_s.at[t])
    wait_bytes(wo_ref, vd_s.at[TILES])
    for g in range(3):
        first, count = GROUPS[g]
        for k in range(1, 4):
            wait_bytes(ov.at[k, :, pl.ds(first * HEAD_DIM, count * HEAD_DIM)], op_s.at[3 * g + order[k] - 1])

    def sent(ref, sems):
        for s in steps:
            @pl.when((z <= 2) & (z >= s - 1))
            def _():
                wait_bytes(ref, sems.at[0, s - 1])

            @pl.when((z >= 1) & (z + s - 1 <= 3))
            def _():
                wait_bytes(ref, sems.at[1, s - 1])

    for i in range(items):
        wait_bytes(xall.at[item_span(i, sp, yp), :], xd_s.at[i])
        sent(x_block(i, z), xz_s.at[i])
    for g in range(3):
        for j in range(4):
            sent(o_block(g, j, z), oz_s.at[4 * g + j])


def attention_block(x, seg, w, wo):
    rows, cols = x.shape
    depth, group = w.shape[0], w.shape[1] // 4
    o_depth, out_cols = wo.shape
    tokens = 4 * rows
    unit = rows // 16
    items = 2 * PIECES - FIRST
    width = HEADS * HEAD_DIM
    chunks = W_BASE[2] + 2 * CHUNKS[2]
    any_space = pl.BlockSpec(memory_space=pl.ANY)
    longest = max(SHARES[0] + SHARES[1], sum(SHARES[FIRST:])) * unit
    longest = max(longest, tokens // QKV_STEPS)

    def dma(*shape):
        return pltpu.SemaphoreType.DMA(shape)

    y, _, _ = pl.pallas_call(
        block_kernel,
        out_shape=(
            jax.ShapeDtypeStruct((rows // 4, 4 * out_cols), jnp.bfloat16),
            jax.ShapeDtypeStruct((tokens, 4 * cols), jnp.bfloat16),
            jax.ShapeDtypeStruct((4 * o_depth, out_cols), jnp.bfloat16),
        ),
        in_specs=[any_space] * 4,
        out_specs=(any_space,) * 3,
        scratch_shapes=[
            pltpu.VMEM((2, longest, 4 * cols), jnp.bfloat16),
            pltpu.VMEM((4 * max(depth, o_depth), group), jnp.bfloat16),
            pltpu.VMEM((tokens, group), jnp.bfloat16),
            pltpu.VMEM((rows, 4 * o_depth), jnp.bfloat16),
            pltpu.VMEM((4, rows, width), jnp.bfloat16),
            pltpu.VMEM((rows, max(cols, out_cols)), jnp.bfloat16),
            pltpu.VMEM((4,) + seg.shape, jnp.int32),
            pltpu.VMEM((tokens, HEAD_DIM), jnp.int32),
            pltpu.VMEM((1, tokens), jnp.int32),
            dma(7),
            dma(3), dma(3),
            dma(PIECES), dma(PIECES), dma(items, 2, 3), dma(items, 2, 3), dma(items + FIRST), dma(items + FIRST),
            dma(chunks), dma(chunks), dma(chunks), dma(6), dma(2), dma(2),
            dma(9), dma(9), dma(12, 2, 3), dma(12, 2, 3),
            dma(2 * TILES), dma(2 * TILES), dma(2 * TILES), dma(2 * TILES), dma(TILES + 1), dma(TILES + 1), dma(TILES),
            dma(3), dma(3),
        ],
        compiler_params=pltpu.CompilerParams(collective_id=0, has_side_effects=True, vmem_limit_bytes=VMEM_LIMIT),
        name="attention_block",
    )(x, seg, w, wo)
    return y


def solution(mesh):
    shape = dict(mesh.shape)
    assert shape == {"dp": 2, "tp": 4, "sp": 4}

    def device_block(x_block, doc_block, wqkv_block, wout_block):
        return attention_block(x_block, doc_block.reshape(-1, HEAD_DIM), wqkv_block, wout_block)

    return jax.shard_map(
        device_block,
        mesh=mesh,
        in_specs=(P(("dp", "sp"), "tp"), P(("dp", "sp")), P("sp", "tp"), P("sp", "tp")),
        out_specs=P(("dp", "sp", "tp"), None),
        check_vma=False,
    )
```

```python
import jax
import jax.numpy as jnp
from jax import lax
from jax.experimental import pallas as pl
from jax.experimental.pallas import tpu as pltpu
from jax.sharding import PartitionSpec as P

HEAD_DIM = 128
HEAD_COLS = 3 * HEAD_DIM
SOFTMAX_SCALE = HEAD_DIM ** -0.5
LOG2_E = 1.4426950408889634
MESH = pl.DeviceIdType.MESH
VMEM_LIMIT = 67_000_000

PIECES = 4
FIRST = 2
SHARES = (5, 4, 4, 3)
HEADS = 4
GROUPS = ((0, 2), (2, 1), (3, 1))
CHUNKS = (4, 2, 2)
W_BASE = (0, 8, 12)
TILES = 4
PARTS = 4
QKV_STEPS = 8


def send(src, dst, ssem, rsem, **device):
    copy = pltpu.make_async_remote_copy(
        src_ref=src, dst_ref=dst, send_sem=ssem, recv_sem=rsem, device_id=device, device_id_type=MESH
    )
    copy.start()


def local(src, dst, sem):
    copy = pltpu.make_async_copy(src, dst, sem)
    copy.start()
    return copy


def wait_bytes(ref, sem):
    pltpu.make_async_copy(ref, ref, sem).wait()


def enter(peers):
    barrier = pltpu.get_barrier_semaphore()
    for peer in peers:
        pl.semaphore_signal(barrier, inc=1, device_id=peer, device_id_type=MESH)
    pl.semaphore_wait(barrier, len(peers))


def aligned(index, size):
    return pl.ds(pl.multiple_of(index * size, size), size)


def columns(start, size):
    return pl.ds(pl.multiple_of(start, HEAD_DIM), size)


def attend(q, k, v, same):
    scores = lax.dot_general(q, k, (((1,), (1,)), ((), ())), preferred_element_type=jnp.float32)
    scores = jnp.where(same, scores, -jnp.inf)
    top = jnp.max(scores, axis=1, keepdims=True)
    weights = jnp.exp2((scores - top) * (SOFTMAX_SCALE * LOG2_E))
    inverse = 1.0 / jnp.sum(weights, axis=1, keepdims=True)
    weights = (weights * inverse).astype(jnp.bfloat16)
    return jnp.dot(weights, v, preferred_element_type=jnp.float32).astype(jnp.bfloat16)


def block_kernel(x_ref, seg_ref, w_ref, wo_ref, y_ref, xall, woall,
                 xs, wf, qv, of, ov, stage, segs, segcol, segrow,
                 loc, seg_s, seg_r, xy_s, xy_r, xz_s, xz_r, xd_s, xd_r,
                 wy_s, wy_r, wx_s, wx_r, wd_s, wd_r,
                 op_s, op_r, oz_s, oz_r,
                 vy_s, vy_r, vx_s, vx_r, vd_s, vd_r, vl, f_s, f_r):
    dp, z, sp = lax.axis_index("dp"), lax.axis_index("tp"), lax.axis_index("sp")
    core, y = lax.rem(sp, 2), sp // 2
    cp, yp, ycp = sp + 1 - 2 * core, lax.rem(sp + 2, 4), 3 - sp
    xp = 1 - dp
    sources = (sp, cp, yp, ycp)
    steps = (1, 2, 3)
    rows, cols = x_ref.shape
    tokens = 4 * rows
    depth = w_ref.shape[0]
    half = depth // 2
    width = HEADS * HEAD_DIM
    unit = rows // 16
    sizes = [share * unit for share in SHARES]
    offsets = [sum(sizes[:i]) for i in range(PIECES)]
    late = PIECES - FIRST
    items = PIECES + late

    def span(owner, i, count=1):
        return pl.ds(pl.multiple_of(owner * rows + offsets[i], unit), sum(sizes[i:i + count]))

    def item_span(i, own, across):
        return span(own, i) if i < PIECES else span(across, FIRST + i - PIECES)

    def x_block(i, k):
        return xall.at[item_span(i, sp, yp), aligned(k, cols)]

    def x_source(i, k, own):
        return x_ref.at[pl.ds(offsets[i], sizes[i]), :] if own and i < PIECES else x_block(i, k)

    def x_core(i, k, own=False):
        send(x_source(i, k, own), x_block(i, k), xd_s.at[i], xd_r.at[i], sp=cp)

    def line_send(copy, s_sem, r_sem, d, s):
        if d == 0:
            @pl.when((z <= 2) & (z >= s - 1))
            def _():
                k = z - (s - 1)
                send(copy[0](k), copy[1](k), s_sem.at[d, s - 1], r_sem.at[d, s - 1], tp=z + 1)
        else:
            @pl.when((z >= 1) & (z + s - 1 <= 3))
            def _():
                k = z + (s - 1)
                send(copy[0](k), copy[1](k), s_sem.at[d, s - 1], r_sem.at[d, s - 1], tp=z - 1)

    def x_line(i, d, s):
        line_send((lambda k: x_source(i, k, s == 1), lambda k: x_block(i, k)), xz_s.at[i], xz_r.at[i], d, s)

    def x_first(i):
        x_line(i, 0, 1)
        x_line(i, 1, 1)

    def x_recv(i, s):
        @pl.when(z >= s)
        def _():
            wait_bytes(x_block(i, z - s), xz_r.at[i, 0, s - 1])
            if s < 3:
                x_line(i, 0, s + 1)
            x_core(i, z - s)

        @pl.when(z + s <= 3)
        def _():
            wait_bytes(x_block(i, z + s), xz_r.at[i, 1, s - 1])
            if s < 3:
                x_line(i, 1, s + 1)
            x_core(i, z + s)

    def p_recv(j):
        wait_bytes(x_block(PIECES + j, z), xy_r.at[j])
        x_core(PIECES + j, z)

    def q_send(i):
        ref = xall.at[span(sp, i), :]
        send(ref, ref, xy_s.at[late + i], xy_r.at[late + i], sp=yp)

    def q_recv(i):
        ref = xall.at[span(yp, i), :]
        wait_bytes(ref, xy_r.at[late + i])
        send(ref, ref, xd_s.at[items + i], xd_r.at[items + i], sp=cp)

    def from_core(i):
        where = item_span(i, cp, ycp) if i < items else span(ycp, i - items)
        wait_bytes(xall.at[where, :], xd_r.at[i])

    def group_cols(g, owner=0):
        first, count = GROUPS[g]
        return columns((owner * HEADS + first) * HEAD_COLS, count * HEAD_COLS)

    def w_rows(quarter, x_half, g, c):
        return aligned((quarter * 2 + x_half) * CHUNKS[g] + c, half // CHUNKS[g])

    def w_send(g):
        for c in range(2 * CHUNKS[g]):
            target = (yp, ycp)[c % 2]
            send(w_ref.at[aligned(dp * CHUNKS[g] + c // 2, half // CHUNKS[g]), group_cols(g, target)],
                 wf.at[w_rows(sp, dp, g, c // 2), group_cols(g)],
                 wy_s.at[W_BASE[g] + c], wy_r.at[W_BASE[g] + c], sp=target)

    def w_recv(g, c):
        ref = wf.at[w_rows((yp, ycp)[c % 2], dp, g, c // 2), group_cols(g)]
        wait_bytes(ref, wy_r.at[W_BASE[g] + c])
        send(ref, ref, wx_s.at[W_BASE[g] + c], wx_r.at[2 * g + c % 2], dp=xp)

    def w_ready(g):
        for n, source in enumerate((yp, ycp)):
            wait_bytes(wf.at[aligned(source * 2 + xp, half), group_cols(g)], wx_r.at[2 * g + n])

    split = (columns(0, 2 * HEAD_COLS), columns(2 * HEAD_COLS, 2 * HEAD_COLS))

    def w_core(n):
        send(w_ref.at[:, columns((cp * HEADS + 2 * n) * HEAD_COLS, 2 * HEAD_COLS)],
             wf.at[aligned(sp, depth), split[n]], wd_s.at[n], wd_r.at[n], sp=cp)

    def w_from_core(n):
        wait_bytes(wf.at[aligned(cp, depth), split[n]], wd_r.at[n])

    def load(where, slot):
        local(xall.at[where, :], xs.at[slot, pl.ds(0, where.size), :], loc.at[4 + slot])

    def go(where, slot):
        size = where.size
        wait_bytes(xs.at[slot, pl.ds(0, size), :], loc.at[4 + slot])

        def step(n, carry):
            at = aligned(n, 2 * HEAD_DIM)
            qv[where, at] = jnp.dot(xs[slot, 0:size, :], wf[0:4 * depth, at],
                                    preferred_element_type=jnp.float32).astype(jnp.bfloat16)
            return carry

        lax.fori_loop(0, GROUPS[0][1] * HEAD_COLS // (2 * HEAD_DIM), step, 0)

    def qkv(where, slot):
        load(where, slot)
        go(where, slot)

    def at_step(n, events):
        for k, acts in events.items():
            @pl.when(n == k)
            def _():
                for act, *args in acts:
                    act(*args)

    part = tokens // QKV_STEPS

    def qkv_group(g, events):
        first, count = GROUPS[g]
        at = pl.ds(first * HEAD_COLS, count * HEAD_COLS)
        load(aligned(0, part), 0)

        def step(n, carry):
            slot = lax.rem(n, 2)

            @pl.when(n + 1 < QKV_STEPS)
            def _():
                local(xall.at[aligned(n + 1, part), :], xs.at[1 - slot, pl.ds(0, part), :], loc.at[5 - slot])

            wait_bytes(xs.at[slot, pl.ds(0, part), :], loc.at[4 + slot])
            qv[aligned(n, part), at] = jnp.dot(xs[slot, 0:part, :], wf[0:4 * depth, at],
                                               preferred_element_type=jnp.float32).astype(jnp.bfloat16)
            at_step(n, events)
            return carry

        lax.fori_loop(0, QKV_STEPS, step, 0)

    def o_block(g, j, k):
        first, count = GROUPS[g]
        return of.at[:, columns(((k * 4 + sources[j]) * HEADS + first) * HEAD_DIM, count * HEAD_DIM)]

    def o_line(g, j, d, s):
        item = 4 * g + j
        line_send((lambda k: o_block(g, j, k),) * 2, oz_s.at[item], oz_r.at[item], d, s)

    def o_first(g, j):
        o_line(g, j, 0, 1)
        o_line(g, j, 1, 1)

    def o_recv(g, j):
        wait_bytes(o_block(g, j, z), op_r.at[3 * g + j - 1])
        o_first(g, j)

    def o_next(g, j, s):
        @pl.when(z >= s)
        def _():
            wait_bytes(o_block(g, j, z - s), oz_r.at[4 * g + j, 0, s - 1])
            if s < 3:
                o_line(g, j, 0, s + 1)

        @pl.when(z + s <= 3)
        def _():
            wait_bytes(o_block(g, j, z + s), oz_r.at[4 * g + j, 1, s - 1])
            if s < 3:
                o_line(g, j, 1, s + 1)

    queries = min(256, rows)
    spans = rows // queries
    order = (0, 2, 3, 1)

    def attention(g, events):
        first, count = GROUPS[g]
        here = pl.ds(first * HEAD_DIM, count * HEAD_DIM)

        def quarter(n, carry):
            owner = 2 * lax.rem(y + lax.rem((n + 1) // 2, 2), 2) + lax.rem(core + n // 2, 2)

            def step(t, carry):
                h, b = first + t // spans, lax.rem(t, spans)
                at = aligned(owner * spans + b, queries)
                ov[n, aligned(b, queries), aligned(h, HEAD_DIM)] = attend(
                    qv[at, aligned(3 * h, HEAD_DIM)], qv[:, aligned(3 * h + 1, HEAD_DIM)],
                    qv[:, aligned(3 * h + 2, HEAD_DIM)], segcol[at, 0:1] == segrow[...])
                return carry

            lax.fori_loop(0, count * spans, step, 0)

            @pl.when(n == 0)
            def _():
                of[:, columns(((z * 4 + sp) * HEADS + first) * HEAD_DIM, count * HEAD_DIM)] = ov[0, :, here]
                o_first(g, 0)

            for k in range(1, 4):
                @pl.when(n == k)
                def _():
                    j = order[k]
                    send(ov.at[k, :, here], o_block(g, 0, z), op_s.at[3 * g + j - 1], op_r.at[3 * g + j - 1],
                         sp=sources[j])

            at_step(n, events)
            return carry

        lax.fori_loop(0, 4, quarter, 0)

    o_depth, out_cols = wo_ref.shape
    o_half = o_depth // 2
    tile = out_cols // TILES

    def v_block(quarter, x_half, c):
        return (aligned((quarter * 2 + x_half) * PARTS + c % PARTS, o_half // PARTS), pl.ds(c // PARTS * tile, tile))

    def v_send(c):
        at = v_block(sp, dp, c)
        send(wo_ref.at[aligned(dp * PARTS + c % PARTS, o_half // PARTS), pl.ds(c // PARTS * tile, tile)], woall.at[at],
             vy_s.at[c], vy_r.at[c], sp=yp)

    def v_recv(c):
        ref = woall.at[v_block(yp, dp, c)]
        wait_bytes(ref, vy_r.at[c])
        send(ref, ref, vx_s.at[c], vx_r.at[c], dp=xp)
        send(ref, ref, vd_s.at[c // PARTS], vd_r.at[c // PARTS], sp=cp)

    def v_from_x(c):
        ref = woall.at[v_block(yp, xp, c)]
        wait_bytes(ref, vx_r.at[c])
        send(ref, ref, vd_s.at[c // PARTS], vd_r.at[c // PARTS], sp=cp)

    def v_place(t):
        return pl.ds(t % 3 * tile, tile)

    def v_load(t):
        at = pl.ds(t * tile, tile)
        wait_bytes(woall.at[aligned(ycp, o_depth), at], vd_r.at[t])
        local(wo_ref.at[:, at], wf.at[aligned(sp, o_depth), v_place(t)], vl.at[t])
        for source in (cp, yp, ycp):
            local(woall.at[aligned(source, o_depth), at], wf.at[aligned(source, o_depth), v_place(t)], vl.at[t])

    piece = rows // 4
    narrow = min(tile, 2 * HEAD_DIM)

    def project(t):
        wait_bytes(wf.at[pl.ds(0, 4 * o_depth), v_place(t)], vl.at[t])

        def step(n, carry):
            stage[:, columns(t * tile + n * narrow, narrow)] = jnp.dot(
                of[...], wf[0:4 * o_depth, columns(t % 3 * tile + n * narrow, narrow)],
                preferred_element_type=jnp.float32).astype(jnp.bfloat16)
            return carry

        lax.fori_loop(0, tile // narrow, step, 0)
        at = pl.ds(t * tile, tile)
        there = columns(z * out_cols + t * tile, tile)
        for r in (2, 1, 3):
            to = lax.rem(z + r, 4)
            send(stage.at[aligned(to, piece), at], y_ref.at[:, there], f_s.at[r - 1], f_r.at[r - 1], tp=to)
        local(stage.at[aligned(z, piece), at], y_ref.at[:, there], loc.at[6])

    x_in = local(x_ref, stage.at[:, pl.ds(0, cols)], loc.at[0])
    w_own = local(w_ref.at[:, columns(sp * HEADS * HEAD_COLS, HEADS * HEAD_COLS)], wf.at[aligned(sp, depth), :],
                  loc.at[2])
    seg_own = local(seg_ref, segs.at[sp], loc.at[3])
    enter([{"sp": cp}, {"sp": yp}, {"sp": ycp}, {"dp": xp}] + [{"tp": lax.rem(z + r, 4)} for r in (1, 2, 3)])
    for n, peer in enumerate((cp, yp, ycp)):
        send(seg_ref, segs.at[sp], seg_s.at[n], seg_r.at[n], sp=peer)
    for j in range(late):
        i = FIRST + j
        send(x_source(i, z, True), x_block(i, z), xy_s.at[j], xy_r.at[j], sp=yp)
    for i in range(FIRST):
        x_first(i)
    w_send(0)
    for i in range(PIECES):
        x_core(i, z, True)
    w_core(0)
    x_in.wait()
    x_put = local(stage.at[:, pl.ds(0, cols)], xall.at[aligned(sp, rows), aligned(z, cols)], loc.at[1])

    x_put.wait()

    chunk = iter(range(2 * CHUNKS[0]))
    for s in steps:
        for i in range(FIRST):
            x_recv(i, s)
            if s == 1:
                p_recv(i)
            else:
                w_recv(0, next(chunk))
            if s == 2:
                w_recv(0, next(chunk))
            if s == 3:
                q_send(i)
        if s == 2:
            for i in range(FIRST, items):
                x_first(i)
    w_send(1)
    for c in chunk:
        w_recv(0, c)
    w_core(1)
    w_own.wait()
    w_from_core(0)
    w_ready(0)
    seg_own.wait()
    for n, peer in enumerate((cp, yp, ycp)):
        wait_bytes(segs.at[peer], seg_r.at[n])
    seg_rows = rows // HEAD_DIM
    for q in range(4):
        for r in range(seg_rows):
            line = segs[q, r:r + 1, :]
            at = (q * seg_rows + r) * HEAD_DIM
            segrow[:, at:at + HEAD_DIM] = line
            segcol[at:at + HEAD_DIM, :] = jnp.broadcast_to(line, (HEAD_DIM, HEAD_DIM)).T
    early = range(FIRST)
    after = range(FIRST, PIECES)
    across = range(PIECES, items)
    qkv(span(sp, 0, FIRST), 0)
    for i in after:
        x_recv(i, 1)
    for i in early:
        from_core(i)
    qkv(span(cp, 0, FIRST), 1)
    for i in across:
        x_recv(i, 1)
    for i in after:
        x_recv(i, 2)
    q_recv(0)
    for i in across:
        x_recv(i, 2)
    qkv(span(yp, 0), 0)
    from_core(items)
    qkv(span(ycp, 0), 1)
    for i in after:
        x_recv(i, 3)
    for i in after:
        from_core(i)
    qkv(span(sp, FIRST, late), 0)
    qkv(span(cp, FIRST, late), 1)
    x_recv(across[0], 3)
    q_recv(1)
    load(span(yp, 1), 0)
    load(span(yp, 2), 1)
    go(span(yp, 1), 0)
    from_core(items + 1)
    load(span(ycp, 1), 0)
    go(span(yp, 2), 1)
    from_core(across[0])
    load(span(ycp, 2), 1)
    x_recv(across[1], 3)
    go(span(ycp, 1), 0)
    load(span(yp, 3), 0)
    go(span(ycp, 2), 1)
    from_core(across[1])
    load(span(ycp, 3), 1)
    go(span(yp, 3), 0)
    go(span(ycp, 3), 1)

    def spread(start, every, acts):
        return {start + every * i: [act] for i, act in enumerate(acts)}

    def weights(g):
        return [(w_recv, g, c) for c in range(2 * CHUNKS[g])]

    def pieces(g, upto):
        return [(o_next, g, j, s) for s in range(1, upto + 1) for j in order]

    def run(acts):
        for act, *args in acts:
            act(*args)

    own = [(o_next, 0, 0, s) for s in steps]
    rest = [(o_next, 0, j, s) for s in steps for j in order[1:]]
    chunks = weights(1)
    attention(0, {0: chunks[:2], 1: own[:1] + chunks[2:3], 2: [(w_send, 2)] + own[1:2] + chunks[3:]})
    for j in order[1:3]:
        o_recv(0, j)
    run(own[2:])
    o_recv(0, order[3])
    w_from_core(1)
    w_ready(1)
    chunks = weights(2)
    qkv_group(1, spread(0, 2, rest[:4]) | spread(3, 2, chunks[:2]))
    rest = rest[4:]
    wo_chunks = [(v_send, c) for c in range(PARTS * TILES)]
    attention(1, {0: chunks[2:3], 2: wo_chunks[:6] + chunks[3:], 3: rest[:2]})
    send(wo_ref, woall.at[aligned(sp, o_depth), :], vd_s.at[TILES], vd_r.at[TILES], sp=cp)
    run(rest[2:3])
    for j in (1, 2, 3):
        o_recv(1, j)
    run(rest[3:-1])
    w_ready(2)
    follow = rest[-1:] + pieces(1, 3)
    blocks = [(v_recv, c) for c in range(PARTS * TILES)]
    plan = spread(0, 1, follow[:QKV_STEPS])
    plan[4] += blocks[:2]
    qkv_group(2, plan)
    follow = follow[QKV_STEPS:]
    attention(2, {0: blocks[2:4], 1: follow[:1], 2: wo_chunks[6:], 3: follow[1:2] + blocks[4:6]})
    run(follow[2:-1])
    for j in order[:0:-1]:
        o_recv(2, j)
    run(follow[-1:])

    crossed = [(W_BASE[g] + c, g) for g in range(len(GROUPS)) for c in range(2 * CHUNKS[g])]
    for c, g in crossed:
        wait_bytes(wf.at[pl.ds(0, half // CHUNKS[g]), group_cols(g)], wx_s.at[c])
    wait_bytes(woall.at[aligned(cp, o_depth), :], vd_r.at[TILES])

    def ready(t):
        for c in range(PARTS):
            v_from_x(PARTS * t + c)
        v_load(t)

    follow = pieces(2, 3)
    run(follow[:4])
    ready(0)
    run(blocks[6:8] + follow[4:8] + blocks[8:10])
    ready(1)
    run(follow[8:])
    project(0)
    run(blocks[10:12])
    project(1)
    run(blocks[12:14])
    ready(2)
    run(blocks[14:])
    project(2)
    ready(3)
    project(3)

    for r in (1, 2, 3):
        wait_bytes(y_ref.at[:, aligned(lax.rem(z + 4 - r, 4), out_cols)], f_r.at[r - 1])
        wait_bytes(stage.at[aligned(z, piece), :], f_s.at[r - 1])
    wait_bytes(y_ref.at[:, aligned(z, out_cols)], loc.at[6])
    for n in range(3):
        wait_bytes(seg_ref, seg_s.at[n])
    for j in range(late):
        wait_bytes(x_block(FIRST + j, z), xy_s.at[j])
    for i in range(FIRST):
        wait_bytes(xall.at[span(sp, i), :], xy_s.at[late + i])
        wait_bytes(xall.at[span(yp, i), :], xd_s.at[items + i])
    for c, g in crossed:
        wait_bytes(wf.at[pl.ds(0, half // CHUNKS[g]), group_cols(g)], wy_s.at[c])
    for n in range(2):
        wait_bytes(wf.at[aligned(sp, depth), split[n]], wd_s.at[n])
    for c in range(PARTS * TILES):
        ref = woall.at[v_block(yp, dp, c)]
        wait_bytes(ref, vy_s.at[c])
        wait_bytes(ref, vx_s.at[c])
    for t in range(TILES):
        wait_bytes(woall.at[aligned(yp, o_depth), pl.ds(t * tile, tile)], vd_s.at[t])
    wait_bytes(wo_ref, vd_s.at[TILES])
    for g in range(3):
        first, count = GROUPS[g]
        for k in range(1, 4):
            wait_bytes(ov.at[k, :, pl.ds(first * HEAD_DIM, count * HEAD_DIM)], op_s.at[3 * g + order[k] - 1])

    def sent(ref, sems):
        for s in steps:
            @pl.when((z <= 2) & (z >= s - 1))
            def _():
                wait_bytes(ref, sems.at[0, s - 1])

            @pl.when((z >= 1) & (z + s - 1 <= 3))
            def _():
                wait_bytes(ref, sems.at[1, s - 1])

    for i in range(items):
        wait_bytes(xall.at[item_span(i, sp, yp), :], xd_s.at[i])
        sent(x_block(i, z), xz_s.at[i])
    for g in range(3):
        for j in range(4):
            sent(o_block(g, j, z), oz_s.at[4 * g + j])


def attention_block(x, seg, w, wo):
    rows, cols = x.shape
    depth, group = w.shape[0], w.shape[1] // 4
    o_depth, out_cols = wo.shape
    tokens = 4 * rows
    unit = rows // 16
    items = 2 * PIECES - FIRST
    width = HEADS * HEAD_DIM
    chunks = W_BASE[2] + 2 * CHUNKS[2]
    any_space = pl.BlockSpec(memory_space=pl.ANY)
    longest = max(SHARES[0] + SHARES[1], sum(SHARES[FIRST:])) * unit
    longest = max(longest, tokens // QKV_STEPS)

    def dma(*shape):
        return pltpu.SemaphoreType.DMA(shape)

    y, _, _ = pl.pallas_call(
        block_kernel,
        out_shape=(
            jax.ShapeDtypeStruct((rows // 4, 4 * out_cols), jnp.bfloat16),
            jax.ShapeDtypeStruct((tokens, 4 * cols), jnp.bfloat16),
            jax.ShapeDtypeStruct((4 * o_depth, out_cols), jnp.bfloat16),
        ),
        in_specs=[any_space] * 4,
        out_specs=(any_space,) * 3,
        scratch_shapes=[
            pltpu.VMEM((2, longest, 4 * cols), jnp.bfloat16),
            pltpu.VMEM((4 * max(depth, o_depth), group), jnp.bfloat16),
            pltpu.VMEM((tokens, group), jnp.bfloat16),
            pltpu.VMEM((rows, 4 * o_depth), jnp.bfloat16),
            pltpu.VMEM((4, rows, width), jnp.bfloat16),
            pltpu.VMEM((rows, max(cols, out_cols)), jnp.bfloat16),
            pltpu.VMEM((4,) + seg.shape, jnp.int32),
            pltpu.VMEM((tokens, HEAD_DIM), jnp.int32),
            pltpu.VMEM((1, tokens), jnp.int32),
            dma(7),
            dma(3), dma(3),
            dma(PIECES), dma(PIECES), dma(items, 2, 3), dma(items, 2, 3), dma(items + FIRST), dma(items + FIRST),
            dma(chunks), dma(chunks), dma(chunks), dma(6), dma(2), dma(2),
            dma(9), dma(9), dma(12, 2, 3), dma(12, 2, 3),
            *[dma(PARTS * TILES)] * 4, dma(TILES + 1), dma(TILES + 1), dma(TILES),
            dma(3), dma(3),
        ],
        compiler_params=pltpu.CompilerParams(collective_id=0, has_side_effects=True, vmem_limit_bytes=VMEM_LIMIT),
        name="attention_block",
    )(x, seg, w, wo)
    return y


def solution(mesh):
    shape = dict(mesh.shape)
    assert shape == {"dp": 2, "tp": 4, "sp": 4}

    def device_block(x_block, doc_block, wqkv_block, wout_block):
        return attention_block(x_block, doc_block.reshape(-1, HEAD_DIM), wqkv_block, wout_block)

    return jax.shard_map(
        device_block,
        mesh=mesh,
        in_specs=(P(("dp", "sp"), "tp"), P(("dp", "sp")), P("sp", "tp"), P("sp", "tp")),
        out_specs=P(("dp", "sp", "tp"), None),
        check_vma=False,
    )
```
